32 devices in a mesh: tiles: 2 (over x), rows: 8 (over z, y), dates: 2 (over core).
Axes of the slice: x: 2, y: 2, z: 4, core: 2. Of those that a mesh axis runs over, the one named last changes fastest.
Arguments:
- red_band: int32 [24, 512, 2048], P('dates', ('tiles', 'rows')), parts along dimension 1, may hold values from 1 to 1073741823
- nir_band: int32 [24, 512, 2048], P('dates', ('tiles', 'rows')), parts along dimension 1, may hold values from 1 to 1073741823
- cloud_class: int32 [24, 512, 2048], P('dates', ('tiles', 'rows')), parts along dimension 1, may hold values from 0 to 3
- date_ordinal: int32 [48], P(('tiles', 'dates')), parts along dimension 0, may hold values from 0 to 23, each once
Outputs:
- composite_red: int32 [512, 2048], P(('tiles', 'rows', 'dates')), parts along dimension 0
- composite_nir: int32 [512, 2048], P(('tiles', 'rows', 'dates')), parts along dimension 0
- chosen_date: int32 [512, 2048], P(('tiles', 'rows', 'dates')), parts along dimension 0
- overview_one: float32 [2, 256, 1024], P(None, ('tiles', 'rows', 'dates')), parts along dimension 1
- overview_two: float32 [2, 128, 512], P(None, ('tiles', 'rows', 'dates')), parts along dimension 1
- overview_three: float32 [2, 64, 256], P(None, ('tiles', 'rows', 'dates')), parts along dimension 1
The draws below stay inside these ranges and needn't reach their ends.
There are 2 independent parts, one for each index of `tiles`. The reference program is written for one: setup_inputs(seed, part) draws one part's arguments, and reference() takes and returns one part's arrays. A program takes and returns all parts, laid end to end along the dimension named above; each array names one. Nothing has to cross between parts.
Inputs may be any that keep to these rules, and one draw needn't show every extreme that they name: `date_ordinal`: each ordinal appears once.
All inputs are finite; a program needn't handle non-finite values.
Results may differ from the reference program's by a relative error of at most 0.0003.
Values sent between devices are 32-bit elements; how exact they have to be, the bound alone decides.
A program may use at most 192 MiB of HBM per device.

```python
import jax
import jax.numpy as jnp
from jax import lax

DATES = 24
W = 2048
LEVELS = 3
ROWS = 256


def draw_bands(key):
    base = jax.random.fold_in(key, 7101)
    keys = jax.random.split(base, 10)
    shape = (DATES, ROWS, W)
    plane = (ROWS, W)
    free_red = jax.random.randint(keys[0], shape, 1, 1073741824, dtype=jnp.int32)
    free_nir = jax.random.randint(keys[1], shape, 1, 1073741824, dtype=jnp.int32)
    kind = jax.random.randint(keys[2], plane, 0, 4, dtype=jnp.int32)[None]
    joined_code = jax.random.randint(keys[3], shape, 0, 16, dtype=jnp.int32)
    joined = joined_code % 2 == 1
    offset = joined_code // 2
    pair = jax.random.randint(keys[4], plane, 0, 4, dtype=jnp.int32)[None]
    table_red = jnp.where(pair == 2, 2, 1).astype(jnp.int32)
    table_nir = jnp.where(pair == 0, 39, jnp.where(pair == 1, 49, jnp.where(pair == 2, 97, 99))).astype(jnp.int32)
    factor = jax.random.randint(keys[5], shape, 1, 10737418, dtype=jnp.int32)
    near_red = jax.random.randint(keys[6], plane, 16777216, 33554432, dtype=jnp.int32)[None]
    near_nir = jax.random.randint(keys[7], plane, 1006632960, 1073741808, dtype=jnp.int32)[None]
    copy_red = jax.random.randint(keys[8], plane, 4194304, 8388608, dtype=jnp.int32)[None]
    copy_nir = jax.random.randint(keys[9], plane, 536870912, 1073741824, dtype=jnp.int32)[None]
    red = jnp.where(joined & (kind == 1), table_red * factor, free_red)
    nir = jnp.where(joined & (kind == 1), table_nir * factor + offset, free_nir)
    red = jnp.where(joined & (kind == 2), near_red + offset, red)
    nir = jnp.where(joined & (kind == 2), near_nir + offset, nir)
    red = jnp.where(joined & (kind == 3), copy_red + jnp.zeros(shape, jnp.int32), red)
    nir = jnp.where(joined & (kind == 3), copy_nir + jnp.zeros(shape, jnp.int32), nir)
    return (red.astype(jnp.int32), nir.astype(jnp.int32))


def draw_red_band(key, part):
    return draw_bands(key)[0]


def draw_nir_band(key, part):
    return draw_bands(key)[1]


def place_ends(drawn, rng, smallest, high):
    index_at = [jax.random.randint(jax.random.fold_in(rng, axis), (), 0, length) for axis, length in enumerate(drawn.shape)]
    longest = drawn.shape.index(max(drawn.shape))
    beside = index_at[:longest] + [(index_at[longest] + 1) % drawn.shape[longest]] + index_at[longest + 1:]
    return drawn.at[tuple(index_at)].set(smallest).at[tuple(beside)].set(high)


def setup_inputs(seed: int = 0, part: int = 0) -> dict:
    key_list = jax.random.split(jax.random.key(seed), 5)
    part_splits = jax.random.split(jax.random.fold_in(key_list[4], part), 5)
    red_band = draw_red_band(jax.random.fold_in(jax.random.fold_in(key_list[4], part), 71), part)
    nir_band = draw_nir_band(jax.random.fold_in(jax.random.fold_in(key_list[4], part), 71), part)
    cloud_class = place_ends(jax.random.randint(part_splits[2], (DATES, ROWS, W), 0, 4), jax.random.fold_in(part_splits[2], 1), 0, 3).astype(jnp.int32)
    date_ordinal = jax.random.permutation(part_splits[3], DATES).astype(jnp.int32)
    return dict(red_band=red_band, nir_band=nir_band, cloud_class=cloud_class, date_ordinal=date_ordinal)


KERNEL = (0.0625, 0.25, 0.375, 0.25, 0.0625)
LIMB = 32768
TWO_LIMBS = 1073741824
SCALE_BAND = 9.313225746154785e-10


def product_digits(small, large):
    small_hi = small // LIMB
    small_lo = small % LIMB
    large_top = large // TWO_LIMBS
    remain = large % TWO_LIMBS
    large_mid = remain // LIMB
    large_lo = remain % LIMB
    digit_zero = small_lo * large_lo
    digit_one = small_hi * large_lo + small_lo * large_mid
    digit_two = small_hi * large_mid + small_lo * large_top
    digit_three = small_hi * large_top
    digit_one = digit_one + digit_zero // LIMB
    digit_zero = digit_zero % LIMB
    digit_two = digit_two + digit_one // LIMB
    digit_one = digit_one % LIMB
    digit_three = digit_three + digit_two // LIMB
    digit_two = digit_two % LIMB
    return (digit_three, digit_two, digit_one, digit_zero)


def compare_digits(first, second):
    greater = first[0] > second[0]
    equal = first[0] == second[0]
    for one, two in zip(first[1:], second[1:]):
        greater = greater | (equal & (one > two))
        equal = equal & (one == two)
    return greater, equal


def better(first, second):
    clear_a, red_a, nir_a, ord_a = first
    clear_b, red_b, nir_b, ord_b = second
    diff_a = nir_a - red_a
    diff_b = nir_b - red_b
    total_a = nir_a + red_a
    total_b = nir_b + red_b
    sign_a = jnp.sign(diff_a)
    sign_b = jnp.sign(diff_b)
    greater, equal = compare_digits(product_digits(jnp.abs(diff_a), total_b), product_digits(jnp.abs(diff_b), total_a))
    lesser = jnp.logical_not(greater | equal)
    same_sign = sign_a == sign_b
    ndvi_more = (sign_a > sign_b) | (same_sign & (((sign_a > 0) & greater) | ((sign_a < 0) & lesser)))
    ndvi_same = same_sign & ((sign_a == 0) | equal)
    same_clear = clear_a == clear_b
    take = (clear_a > clear_b) | (same_clear & (ndvi_more | (ndvi_same & (ord_a < ord_b))))
    return tuple(jnp.where(take, one, two) for one, two in zip(first, second))


def blur_pool(level):
    rows = level.shape[1]
    cols = level.shape[2]
    padded = jnp.pad(level, ((0, 0), (2, 2), (0, 0)))
    smooth = KERNEL[0] * padded[:, 0:rows]
    for offset in range(1, 5):
        smooth = smooth + KERNEL[offset] * padded[:, offset:offset + rows]
    padded = jnp.pad(smooth, ((0, 0), (0, 0), (2, 2)))
    result = KERNEL[0] * padded[:, :, 0:cols]
    for offset in range(1, 5):
        result = result + KERNEL[offset] * padded[:, :, offset:offset + cols]
    return result.reshape(2, rows // 2, 2, cols // 2, 2).mean(axis=(2, 4))


def reference(red_band, nir_band, cloud_class, date_ordinal):
    def entry(index):
        return ((cloud_class[index] == 0).astype(jnp.int32), red_band[index], nir_band[index],
                jnp.full(red_band.shape[1:], date_ordinal[index], jnp.int32))

    def advance(carry, index):
        return better(carry, entry(index)), None

    best, unused = lax.scan(advance, entry(0), jnp.arange(1, DATES, dtype=jnp.int32))
    level = jnp.stack([best[1], best[2]]).astype(jnp.float32) * SCALE_BAND
    levels = []
    for number in range(LEVELS):
        level = blur_pool(level)
        levels.append(level)
    return best[1], best[2], best[3], levels[0], levels[1], levels[2]
```

```python
import jax
import jax.numpy as jnp
import numpy as np
from jax import lax
from jax.experimental import pallas as pl
from jax.experimental.pallas import tpu as pltpu
from jax.sharding import PartitionSpec as P

LEVELS = 3
LIMB_BITS = 15
LIMB_MASK = (1 << LIMB_BITS) - 1
FLAG = 1 << 30
SCALE_BAND = 2.0**-30
LANES = 128
TILE = 8
WIDTH = 512
MESH = pl.DeviceIdType.MESH
TAPS = np.array([1, 5, 10, 10, 5, 1], np.float64) / 32


def taps(distance):
    far = (distance == 0) | (distance == 5)
    mid = (distance == 1) | (distance == 4)
    near = (distance == 2) | (distance == 3)
    return jnp.where(near, 0.3125, jnp.where(mid, 0.15625, jnp.where(far, 0.03125, 0.0)))


def limbs(value):
    return value >> LIMB_BITS, value & LIMB_MASK


def take_first(first, second):
    r1a, r0a, n1a, n0a, clear_a, ord_a = first
    r1b, r0b, n1b, n0b, clear_b, ord_b = second
    low = n0a * r0b - n0b * r0a + ((ord_b - ord_a) >> 31)
    mid = (n1a * r0b + n0a * r1b) - (n1b * r0a + n0b * r1a) + (low >> LIMB_BITS)
    high = n1a * r1b - n1b * r1a + (mid >> LIMB_BITS)
    return high >= clear_b - clear_a


def pick(take, first, second):
    return tuple(jnp.where(take, one, two) for one, two in zip(first, second))


def joined(entry):
    r1, r0, n1, n0, clear, order = entry
    return (r1 << LIMB_BITS) | r0, (n1 << LIMB_BITS) | n0, clear, order


def split(value):
    high = value.astype(jnp.bfloat16)
    return high, (value - high.astype(jnp.float32)).astype(jnp.bfloat16)


def iota(shape, axis):
    return lax.broadcasted_iota(jnp.int32, shape, axis)


def row_weights(own):
    chunk = own // 2
    table = np.zeros((4, 16 * TILE, LANES))
    for core in range(2):
        for outer in range(2):
            def image(r):
                return np.eye(own)[r] if 0 <= r < own else np.zeros(own)

            def inside(level, row):
                count = own >> level
                beyond = row < 0 if core == 0 else row >= count
                return outer == 1 or not beyond

            def level_row(level, row):
                if level == 0:
                    return image(row)
                if not inside(level, row):
                    return np.zeros(own)
                return sum(TAPS[d] * level_row(level - 1, 2 * row - 2 + d) for d in range(6))

            rows = {}
            above = [[-1], [-2, -1], [-2, -1]]
            for level in range(1, LEVELS + 1):
                count = own >> level
                below = [[count], [count, count + 1], [count, count + 1]][level - 1]
                outside, beside = (above[level - 1], below) if core == 0 else (below, above[level - 1])
                first = 0 if level == 1 else 2
                for band in range(2):
                    for base, picked in ((0, outside), (TILE, beside)):
                        for n, row in enumerate(picked):
                            rows[level, base + first + band * len(picked) + n] = (band, level_row(level, row))
                    start = 2 * TILE + (2 if level == 3 else 0)
                    for n in range(count):
                        rows[level, start + band * count + n] = (band, level_row(level, n))
            for (level, m), (band, weights) in rows.items():
                for k in range(4 * own):
                    slot, within = k // (4 * chunk), k % chunk
                    if (k // chunk) % 2 != band:
                        continue
                    place = slot if core == 0 else 1 - slot
                    value = weights[place * chunk + within] * SCALE_BAND
                    top = np.float64(np.asarray(value, jnp.bfloat16))
                    table[2 * core + outer, (level - 1) * 4 * TILE + m, k] = top
                    if level == LEVELS:
                        table[2 * core + outer, level * 4 * TILE + m, k] = value - top
    return table.astype(jnp.bfloat16)


def kernel(
    red, nir, cloud, ordinals, table, out_red, out_nir, out_ord, out_1, out_2, out_3,
    stream, best, arrived, wide_0, wide_1, wide_2, message, received, weights,
    ords, load_sem, order_sem, send_sem, best_sem, sum_sem, pieces,
):
    tile = lax.axis_index("tiles")
    strip_index = lax.axis_index("rows")
    core = lax.axis_index("dates")
    strips = lax.axis_size("rows")
    dates, strip, width = red.shape
    chunk = strip // 4
    half = width // 2
    has_outer = jnp.where(core == 0, strip_index > 0, strip_index < strips - 1)
    outer_strip = jnp.clip(strip_index + 2 * core - 1, 0, strips - 1)
    partner = (tile, strip_index, 1 - core)
    outer = (tile, outer_strip, 1 - core)
    rows_of = [(3 - 3 * core) * chunk, (2 - core) * chunk, 3 * core * chunk, (1 + core) * chunk]

    arrivals = []
    for number, (slot, start, size) in enumerate(pieces):
        begin = pl.multiple_of(rows_of[slot], chunk)
        columns = pl.ds(start, size)
        for band, source in enumerate((red, nir, cloud)):
            pltpu.make_async_copy(
                source.at[:, pl.ds(begin, chunk), columns],
                stream.at[slot, band, :, :, columns],
                load_sem.at[number],
            ).start()
        whole = stream.at[slot, :, :, :, columns]
        arrivals.append(pltpu.make_async_copy(whole, whole, load_sem.at[number]))
    order_copy = pltpu.make_async_copy(ordinals, ords, order_sem.at[0])
    order_copy.start()
    case = 2 * core + has_outer.astype(jnp.int32)
    table_copy = pltpu.make_async_copy(table.at[case], weights, order_sem.at[1])
    table_copy.start()

    barrier = pltpu.get_barrier_semaphore()
    pl.semaphore_signal(barrier, inc=1, device_id=partner, device_id_type=MESH)

    @pl.when(has_outer)
    def _():
        pl.semaphore_signal(barrier, inc=1, device_id=outer, device_id_type=MESH)

    k = iota((4 * LANES, LANES), 0)
    j = iota((4 * LANES, LANES), 1)
    column_weights = taps(k - LANES - (2 * j - 2)).astype(jnp.bfloat16)

    @pl.when(jnp.logical_not(has_outer))
    def _():
        received[0] = jnp.zeros(received.shape[1:], jnp.float32)

    for wide in (wide_0, wide_1, wide_2):
        edge = jnp.zeros((wide.shape[0], LANES), jnp.bfloat16)
        wide[:, 0:LANES] = edge
        wide[:, wide.shape[1] - LANES :] = edge

    order_copy.wait()

    def find_best(slot, start, size, own):
        place = slot - 2

        def step(number, unused):
            at = pl.multiple_of(number * WIDTH + start, WIDTH)
            columns = pl.ds(at, WIDTH)

            def entry(date):
                red_hi, red_lo = limbs(stream[slot, 0, date, :, columns])
                nir_hi, nir_lo = limbs(stream[slot, 1, date, :, columns])
                clear = jnp.where(stream[slot, 2, date, :, columns] == 0, FLAG, 0)
                return (red_hi, red_lo, nir_hi, nir_lo, clear, ords[date])

            current = None
            if own:
                red_hi, red_lo = limbs(arrived[place, 0, :, columns])
                nir_hi, nir_lo = limbs(arrived[place, 1, :, columns])
                packed = arrived[place, 2, :, columns]
                current = (red_hi, red_lo, nir_hi, nir_lo, packed & FLAG, packed & (FLAG - 1))
            for date in range(0, dates, 2):
                other = entry(date)
                if date + 1 < dates:
                    later = entry(date + 1)
                    other = pick(take_first(later, other), later, other)
                current = other if current is None else pick(take_first(other, current), other, current)
            value_red, value_nir, clear, order = joined(current)
            if own:
                out_row = (core if place == 0 else 1 - core) * chunk
                rows = pl.ds(pl.multiple_of(out_row, chunk), chunk)
                out_red[rows, columns] = value_red
                out_nir[rows, columns] = value_nir
                out_ord[rows, columns] = order
                inner = pl.ds(pl.multiple_of(at + LANES, LANES), WIDTH)
                both = jnp.concatenate([value_red, value_nir], axis=0).astype(jnp.float32)
                high, low = split(both)
                base = place * 4 * chunk
                wide_0[base : base + 2 * chunk, inner] = high
                wide_0[base + 2 * chunk : base + 4 * chunk, inner] = low
            else:
                best[slot, 0, :, columns] = value_red
                best[slot, 1, :, columns] = value_nir
                best[slot, 2, :, columns] = clear + order
            return unused

        lax.fori_loop(0, size // WIDTH, step, 0)

    def best_copy(slot, part):
        columns = pl.ds(part * half, half)
        return pltpu.make_async_remote_copy(
            src_ref=best.at[slot, :, :, columns],
            dst_ref=arrived.at[slot, :, :, columns],
            send_sem=send_sem.at[0],
            recv_sem=best_sem.at[slot, part],
            device_id=partner,
            device_id_type=MESH,
        )

    waiting = list(zip(pieces, arrivals))

    def run(slot, part):
        begin, end = part * half, (part + 1) * half
        at = begin
        while at < end:
            if waiting and waiting[0][0][:2] == (slot, at):
                waiting.pop(0)[1].wait()
            stop = min([end] + [piece[1] for piece, _ in waiting if piece[0] == slot and piece[1] > at])
            find_best(slot, at, stop - at, slot >= 2)
            at = stop

    for slot in range(2):
        for part in range(2):
            run(slot, part)
            if slot == 0 and part == 0:
                pl.semaphore_wait(barrier, 1 + has_outer.astype(jnp.int32))
            best_copy(slot, part).start()
    for slot in range(2):
        for part in range(2):
            best_copy(slot, part).wait_recv()
            run(slot + 2, part)
    table_copy.wait()

    def filter_columns(source):
        blocks = (source.shape[1] - 2 * LANES) // (2 * LANES)
        left = jnp.concatenate([source[:, 2 * LANES * b : 2 * LANES * b + 4 * LANES] for b in range(blocks)], axis=0)
        out = jnp.dot(left, column_weights, preferred_element_type=jnp.float32)
        count = source.shape[0]
        group = 2 * chunk
        places = []
        for place in range(2):
            parts = []
            for b in range(blocks):
                row = b * count + place * 2 * group
                parts.append(out[row : row + group] + out[row + group : row + 2 * group])
            places.append(split(jnp.concatenate(parts, axis=1)))
        return jnp.concatenate([value for pair in places for value in pair], axis=0)

    def filter_rows(level, data, count):
        left = weights[(level - 1) * 4 * TILE : ((level - 1) * 4 + count) * TILE, 0 : data.shape[0]]
        return jnp.dot(left, data, preferred_element_type=jnp.float32)

    data_1 = filter_columns(wide_0)
    wide_1[:, LANES : LANES + half] = data_1
    data_2 = filter_columns(wide_1)
    wide_2[:, LANES : LANES + half // 2] = data_2
    data_3 = filter_columns(wide_2)
    level_1 = filter_rows(1, data_1, 4)
    level_2 = filter_rows(2, data_2, 4)
    level_3 = filter_rows(3, data_3, 8)
    level_3 = level_3[0 : 3 * TILE] + level_3[4 * TILE : 7 * TILE]
    ends = (half // 2, half // 2 + half // 4)

    def sums(side):
        rows = slice(side * TILE, (side + 1) * TILE)
        one, two, three = level_1[rows], level_2[rows], level_3[rows]
        message[side, :, 0 : ends[0]] = one[:, 0 : ends[0]] + two
        message[side, :, ends[0] : ends[1]] = one[:, ends[0] : ends[1]] + three
        message[side, :, ends[1] :] = one[:, ends[1] :]

    def sum_copy(side, device):
        return pltpu.make_async_remote_copy(
            src_ref=message.at[side],
            dst_ref=received.at[side],
            send_sem=send_sem.at[1 + side],
            recv_sem=sum_sem.at[side],
            device_id=device,
            device_id_type=MESH,
        )

    to_outer, to_partner = sum_copy(0, outer), sum_copy(1, partner)
    sums(0)

    @pl.when(has_outer)
    def _():
        to_outer.start()

    sums(1)
    to_partner.start()
    to_partner.wait_recv()

    @pl.when(has_outer)
    def _():
        to_outer.wait_recv()

    def spread(side, row, columns):
        return jnp.broadcast_to(received[side, row : row + 1, columns], (TILE, columns.stop - columns.start))

    row = iota((TILE, half), 0)
    edges = ((TILE - 1) * core, (TILE - 1) * (1 - core))
    for band in range(2):
        total = level_1[(2 + band) * TILE : (3 + band) * TILE]
        for side in range(2):
            total = total + jnp.where(row == edges[side], spread(side, band, slice(0, half)), 0.0)
        out_1[band] = total
    row = iota((TILE, ends[0]), 0)
    total = level_2[2 * TILE : 3 * TILE]
    for side in range(2):
        shift = 2 * (core if side == 0 else 1 - core)
        for number in range(4):
            target = number % 2 + 4 * (number // 2) + shift
            total = total + jnp.where(row == target, spread(side, 2 + number, slice(0, ends[0])), 0.0)
    out_2[0] = total[0:4]
    out_2[1] = total[4:8]
    total = level_3[2 * TILE : 3 * TILE] + received[0, :, ends[0] : ends[1]] + received[1, :, ends[0] : ends[1]]
    out_3[0] = total[2:4]
    out_3[1] = total[4:6]

    pltpu.make_async_copy(best, best, send_sem.at[0]).wait()
    to_partner.wait_send()

    @pl.when(has_outer)
    def _():
        to_outer.wait_send()


def write_out(*refs):
    count = len(refs) // 2
    semaphores = refs[-1]
    copies = [pltpu.make_async_copy(refs[n], refs[count + n], semaphores.at[n]) for n in range(count)]
    for copy in copies:
        copy.start()
    for copy in copies:
        copy.wait()


def body(red_band, nir_band, cloud_class, date_ordinal):
    dates, strip, width = red_band.shape
    own = strip // 2
    chunk = strip // 4
    half = width // 2
    whole = pl.BlockSpec(memory_space=pltpu.VMEM)
    anywhere = pl.BlockSpec(memory_space=pl.ANY)
    outs = [jax.ShapeDtypeStruct((own, width), jnp.int32)] * 3
    outs += [jax.ShapeDtypeStruct((2, own >> n, width >> n), jnp.float32) for n in range(1, LEVELS + 1)]
    kept = [pltpu.VMEM(out.shape, out.dtype) for out in outs]
    pieces = [(0, 0, half // 2), (0, half // 2, half // 2), (0, half, half)] + [(slot, 0, width) for slot in range(1, 4)]
    pieces = tuple(pieces)
    table = row_weights(own)

    def run(*refs):
        kernel(*refs, pieces=pieces)

    results = pl.pallas_call(
        run,
        out_shape=kept,
        in_specs=[anywhere] * 5,
        out_specs=[whole] * 6,
        scratch_shapes=[
            pltpu.VMEM((4, 3, dates, chunk, width), jnp.int32),
            pltpu.VMEM((2, 3, chunk, width), jnp.int32),
            pltpu.VMEM((2, 3, chunk, width), jnp.int32),
            pltpu.VMEM((8 * chunk, width + 2 * LANES), jnp.bfloat16),
            pltpu.VMEM((8 * chunk, width // 2 + 2 * LANES), jnp.bfloat16),
            pltpu.VMEM((8 * chunk, width // 4 + 2 * LANES), jnp.bfloat16),
            pltpu.VMEM((2, TILE, half), jnp.float32),
            pltpu.VMEM((2, TILE, half), jnp.float32),
            pltpu.VMEM(table.shape[1:], jnp.bfloat16),
            pltpu.SMEM((dates,), jnp.int32),
            pltpu.SemaphoreType.DMA((len(pieces),)),
            pltpu.SemaphoreType.DMA((2,)),
            pltpu.SemaphoreType.DMA((3,)),
            pltpu.SemaphoreType.DMA((2, 2)),
            pltpu.SemaphoreType.DMA((2,)),
        ],
        compiler_params=pltpu.CompilerParams(collective_id=0, has_side_effects=True),
        name="composite",
    )(red_band, nir_band, cloud_class, date_ordinal, jnp.asarray(table))
    return pl.pallas_call(
        write_out,
        out_shape=outs,
        in_specs=[whole] * 6,
        out_specs=[anywhere] * 6,
        scratch_shapes=[pltpu.SemaphoreType.DMA((6,))],
        name="write_out",
    )(*[pltpu.with_memory_space_constraint(result, pltpu.VMEM) for result in results])


def solution(mesh):
    in_specs = (
        P("dates", ("tiles", "rows"), None),
        P("dates", ("tiles", "rows"), None),
        P("dates", ("tiles", "rows"), None),
        P(("tiles", "dates")),
    )
    out_specs = (
        P(("tiles", "rows", "dates"), None),
        P(("tiles", "rows", "dates"), None),
        P(("tiles", "rows", "dates"), None),
        P(None, ("tiles", "rows", "dates"), None),
        P(None, ("tiles", "rows", "dates"), None),
        P(None, ("tiles", "rows", "dates"), None),
    )
    return jax.shard_map(body, mesh=mesh, in_specs=in_specs, out_specs=out_specs, check_vma=False)
```

```python
import jax
import jax.numpy as jnp
import numpy as np
from jax import lax
from jax.experimental import pallas as pl
from jax.experimental.pallas import tpu as pltpu
from jax.sharding import PartitionSpec as P

LEVELS = 3
LIMB_BITS = 15
LIMB_MASK = (1 << LIMB_BITS) - 1
FLAG = 1 << 30
SCALE_BAND = 2.0**-30
LANES = 128
TILE = 8
WIDTH = 512
MESH = pl.DeviceIdType.MESH
TAPS = np.array([1, 5, 10, 10, 5, 1], np.float64) / 32


def taps(distance):
    far = (distance == 0) | (distance == 5)
    mid = (distance == 1) | (distance == 4)
    near = (distance == 2) | (distance == 3)
    return jnp.where(near, 0.3125, jnp.where(mid, 0.15625, jnp.where(far, 0.03125, 0.0)))


def limbs(value):
    return value >> LIMB_BITS, value & LIMB_MASK


def take_first(first, second):
    r1a, r0a, n1a, n0a, clear_a, ord_a = first
    r1b, r0b, n1b, n0b, clear_b, ord_b = second
    low = n0a * r0b - n0b * r0a + ((ord_b - ord_a) >> 31)
    mid = (n1a * r0b + n0a * r1b) - (n1b * r0a + n0b * r1a) + (low >> LIMB_BITS)
    high = n1a * r1b - n1b * r1a + (mid >> LIMB_BITS)
    return high >= clear_b - clear_a


def pick(take, first, second):
    return tuple(jnp.where(take, one, two) for one, two in zip(first, second))


def joined(entry):
    r1, r0, n1, n0, clear, order = entry
    return (r1 << LIMB_BITS) | r0, (n1 << LIMB_BITS) | n0, clear, order


def split(value):
    high = value.astype(jnp.bfloat16)
    return high, (value - high.astype(jnp.float32)).astype(jnp.bfloat16)


def iota(shape, axis):
    return lax.broadcasted_iota(jnp.int32, shape, axis)


def row_weights(own):
    chunk = own // 2
    table = np.zeros((4, 16 * TILE, LANES))
    for core in range(2):
        for outer in range(2):
            def image(r):
                return np.eye(own)[r] if 0 <= r < own else np.zeros(own)

            def inside(level, row):
                count = own >> level
                beyond = row < 0 if core == 0 else row >= count
                return outer == 1 or not beyond

            def level_row(level, row):
                if level == 0:
                    return image(row)
                if not inside(level, row):
                    return np.zeros(own)
                return sum(TAPS[d] * level_row(level - 1, 2 * row - 2 + d) for d in range(6))

            rows = {}
            above = [[-1], [-2, -1], [-2, -1]]
            for level in range(1, LEVELS + 1):
                count = own >> level
                below = [[count], [count, count + 1], [count, count + 1]][level - 1]
                outside, beside = (above[level - 1], below) if core == 0 else (below, above[level - 1])
                first = 0 if level == 1 else 2
                for band in range(2):
                    for base, picked in ((0, outside), (TILE, beside)):
                        for n, row in enumerate(picked):
                            rows[level, base + first + band * len(picked) + n] = (band, level_row(level, row))
                    start = 2 * TILE + (2 if level == 3 else 0)
                    for n in range(count):
                        rows[level, start + band * count + n] = (band, level_row(level, n))
            for (level, m), (band, weights) in rows.items():
                for k in range(4 * own):
                    slot, within = k // (4 * chunk), k % chunk
                    if (k // chunk) % 2 != band:
                        continue
                    place = slot if core == 0 else 1 - slot
                    value = weights[place * chunk + within] * SCALE_BAND
                    top = np.float64(np.asarray(value, jnp.bfloat16))
                    table[2 * core + outer, (level - 1) * 4 * TILE + m, k] = top
                    if level == LEVELS:
                        table[2 * core + outer, level * 4 * TILE + m, k] = value - top
    return table.astype(jnp.bfloat16)


def kernel(
    red, nir, cloud, ordinals, table, out_red, out_nir, out_ord, out_1, out_2, out_3,
    stream, best, arrived, merged, wide_0, wide_1, wide_2, message, received, home, homed, weights,
    ords, load_sem, order_sem, send_sem, best_sem, sum_sem, pieces,
):
    tile = lax.axis_index("tiles")
    strip_index = lax.axis_index("rows")
    core = lax.axis_index("dates")
    strips = lax.axis_size("rows")
    dates, strip, width = red.shape
    chunk = strip // 4
    half = width // 2
    toward = 1 - 2 * core
    has_target = jnp.where(core == 0, strip_index < strips - 1, strip_index > 0)
    has_source = jnp.where(core == 0, strip_index > 0, strip_index < strips - 1)
    partner = (tile, strip_index, 1 - core)
    target = (tile, jnp.clip(strip_index + toward, 0, strips - 1), core)
    source_device = (tile, jnp.clip(strip_index - toward, 0, strips - 1), core)
    rows_of = [3 * core * chunk, (1 + core) * chunk, (3 - 3 * core) * chunk, (2 - core) * chunk]

    arrivals = []
    for number, (slot, start, size) in enumerate(pieces):
        begin = pl.multiple_of(rows_of[slot], chunk)
        columns = pl.ds(start, size)
        for band, source in enumerate((red, nir, cloud)):
            pltpu.make_async_copy(
                source.at[:, pl.ds(begin, chunk), columns],
                stream.at[slot, band, :, :, columns],
                load_sem.at[number],
            ).start()
        whole = stream.at[slot, :, :, :, columns]
        arrivals.append(pltpu.make_async_copy(whole, whole, load_sem.at[number]))
    order_copy = pltpu.make_async_copy(ordinals, ords, order_sem.at[0])
    order_copy.start()
    case = 2 * (1 - core) + has_target.astype(jnp.int32)
    table_copy = pltpu.make_async_copy(table.at[case], weights, order_sem.at[1])
    table_copy.start()

    barrier = pltpu.get_barrier_semaphore()
    pl.semaphore_signal(barrier, inc=1, device_id=partner, device_id_type=MESH)

    @pl.when(has_source)
    def _():
        pl.semaphore_signal(barrier, inc=1, device_id=source_device, device_id_type=MESH)

    k = iota((4 * LANES, LANES), 0)
    j = iota((4 * LANES, LANES), 1)
    column_weights = taps(k - LANES - (2 * j - 2)).astype(jnp.bfloat16)

    @pl.when(jnp.logical_not(has_source))
    def _():
        received[...] = jnp.zeros(received.shape, jnp.float32)

    for wide in (wide_0, wide_1, wide_2):
        edge = jnp.zeros((wide.shape[0], LANES), jnp.bfloat16)
        wide[:, 0:LANES] = edge
        wide[:, wide.shape[1] - LANES :] = edge

    order_copy.wait()

    def find_best(slot, start, size, own):
        place = slot - 2

        def step(number, unused):
            at = pl.multiple_of(number * WIDTH + start, WIDTH)
            columns = pl.ds(at, WIDTH)

            def entry(date):
                red_hi, red_lo = limbs(stream[slot, 0, date, :, columns])
                nir_hi, nir_lo = limbs(stream[slot, 1, date, :, columns])
                clear = jnp.where(stream[slot, 2, date, :, columns] == 0, FLAG, 0)
                return (red_hi, red_lo, nir_hi, nir_lo, clear, ords[date])

            current = None
            if own:
                red_hi, red_lo = limbs(arrived[place, 0, :, columns])
                nir_hi, nir_lo = limbs(arrived[place, 1, :, columns])
                packed = arrived[place, 2, :, columns]
                current = (red_hi, red_lo, nir_hi, nir_lo, packed & FLAG, packed & (FLAG - 1))
            for date in range(0, dates, 2):
                other = entry(date)
                if date + 1 < dates:
                    later = entry(date + 1)
                    other = pick(take_first(later, other), later, other)
                current = other if current is None else pick(take_first(other, current), other, current)
            value_red, value_nir, clear, order = joined(current)
            if own:
                merged[place, 0, :, columns] = value_red
                merged[place, 1, :, columns] = value_nir
                merged[place, 2, :, columns] = order
                inner = pl.ds(pl.multiple_of(at + LANES, LANES), WIDTH)
                both = jnp.concatenate([value_red, value_nir], axis=0).astype(jnp.float32)
                high, low = split(both)
                base = place * 4 * chunk
                wide_0[base : base + 2 * chunk, inner] = high
                wide_0[base + 2 * chunk : base + 4 * chunk, inner] = low
            else:
                best[slot, 0, :, columns] = value_red
                best[slot, 1, :, columns] = value_nir
                best[slot, 2, :, columns] = clear + order
            return unused

        lax.fori_loop(0, size // WIDTH, step, 0)

    def best_copy(slot, part):
        columns = pl.ds(part * half, half)
        return pltpu.make_async_remote_copy(
            src_ref=best.at[slot, :, :, columns],
            dst_ref=arrived.at[slot, :, :, columns],
            send_sem=send_sem.at[0],
            recv_sem=best_sem.at[slot, part],
            device_id=partner,
            device_id_type=MESH,
        )

    waiting = list(zip(pieces, arrivals))

    def run(slot, part):
        begin, end = part * half, (part + 1) * half
        at = begin
        while at < end:
            if waiting and waiting[0][0][:2] == (slot, at):
                waiting.pop(0)[1].wait()
            stop = min([end] + [piece[1] for piece, _ in waiting if piece[0] == slot and piece[1] > at])
            find_best(slot, at, stop - at, slot >= 2)
            at = stop

    for slot in range(2):
        for part in range(2):
            run(slot, part)
            if slot == 0 and part == 0:
                pl.semaphore_wait(barrier, 1 + has_target.astype(jnp.int32))
            best_copy(slot, part).start()
    for slot in range(2):
        for part in range(2):
            best_copy(slot, part).wait_recv()
            run(slot + 2, part)
        merged_rows = pl.ds(pl.multiple_of(((1 - core) if slot == 0 else core) * chunk, chunk), chunk)
        for number, result in enumerate((out_red, out_nir, out_ord)):
            pltpu.make_async_remote_copy(
                src_ref=merged.at[slot, number],
                dst_ref=result.at[merged_rows],
                send_sem=send_sem.at[1],
                recv_sem=sum_sem.at[0],
                device_id=partner,
                device_id_type=MESH,
            ).start()
    table_copy.wait()

    def filter_columns(source):
        blocks = (source.shape[1] - 2 * LANES) // (2 * LANES)
        left = jnp.concatenate([source[:, 2 * LANES * b : 2 * LANES * b + 4 * LANES] for b in range(blocks)], axis=0)
        out = jnp.dot(left, column_weights, preferred_element_type=jnp.float32)
        count = source.shape[0]
        group = 2 * chunk
        places = []
        for place in range(2):
            parts = []
            for b in range(blocks):
                row = b * count + place * 2 * group
                parts.append(out[row : row + group] + out[row + group : row + 2 * group])
            places.append(split(jnp.concatenate(parts, axis=1)))
        return jnp.concatenate([value for pair in places for value in pair], axis=0)

    def filter_rows(level, data, count):
        left = weights[(level - 1) * 4 * TILE : ((level - 1) * 4 + count) * TILE, 0 : data.shape[0]]
        return jnp.dot(left, data, preferred_element_type=jnp.float32)

    data_1 = filter_columns(wide_0)
    wide_1[:, LANES : LANES + half] = data_1
    data_2 = filter_columns(wide_1)
    wide_2[:, LANES : LANES + half // 2] = data_2
    data_3 = filter_columns(wide_2)
    level_1 = filter_rows(1, data_1, 4)
    level_2 = filter_rows(2, data_2, 4)
    level_3 = filter_rows(3, data_3, 8)
    level_3 = level_3[0 : 3 * TILE] + level_3[4 * TILE : 7 * TILE]
    ends = (half // 2, half // 2 + half // 4)

    def sums(side, held):
        rows = slice(side * TILE, (side + 1) * TILE)
        one, two, three = level_1[rows], level_2[rows], level_3[rows]
        held[:, 0 : ends[0]] = one[:, 0 : ends[0]] + two
        held[:, ends[0] : ends[1]] = one[:, ends[0] : ends[1]] + three
        held[:, ends[1] :] = one[:, ends[1] :]

    to_target = pltpu.make_async_remote_copy(
        src_ref=message.at[0],
        dst_ref=received,
        send_sem=send_sem.at[2],
        recv_sem=sum_sem.at[1],
        device_id=target,
        device_id_type=MESH,
    )
    to_partner = pltpu.make_async_remote_copy(
        src_ref=home,
        dst_ref=homed,
        send_sem=send_sem.at[3],
        recv_sem=sum_sem.at[2],
        device_id=partner,
        device_id_type=MESH,
    )
    sums(0, message.at[0])

    @pl.when(has_target)
    def _():
        to_target.start()

    home[0 : 2 * TILE] = level_1[2 * TILE : 4 * TILE]
    home[2 * TILE :, 0 : ends[0]] = level_2[2 * TILE : 3 * TILE]
    home[2 * TILE :, ends[0] : ends[1]] = level_3[2 * TILE : 3 * TILE]
    home[2 * TILE :, ends[1] :] = jnp.zeros((TILE, half - ends[1]), jnp.float32)
    to_partner.start()
    sums(1, message.at[1])
    to_partner.wait_recv()
    pltpu.make_async_copy(merged, merged, sum_sem.at[0]).wait()

    @pl.when(has_source)
    def _():
        to_target.wait_recv()

    sides = (received, message.at[1])

    def spread(side, row, columns):
        return jnp.broadcast_to(sides[side][row : row + 1, columns], (TILE, columns.stop - columns.start))

    row = iota((TILE, half), 0)
    edges = ((TILE - 1) * core, (TILE - 1) * (1 - core))
    for band in range(2):
        total = homed[band * TILE : (band + 1) * TILE]
        for side in range(2):
            total = total + jnp.where(row == edges[side], spread(side, band, slice(0, half)), 0.0)
        out_1[band] = total
    row = iota((TILE, ends[0]), 0)
    total = homed[2 * TILE :, 0 : ends[0]]
    for side in range(2):
        shift = 2 * (core if side == 0 else 1 - core)
        for number in range(4):
            target = number % 2 + 4 * (number // 2) + shift
            total = total + jnp.where(row == target, spread(side, 2 + number, slice(0, ends[0])), 0.0)
    out_2[0] = total[0:4]
    out_2[1] = total[4:8]
    third = slice(ends[0], ends[1])
    total = homed[2 * TILE :, third] + sides[0][:, third] + sides[1][:, third]
    out_3[0] = total[2:4]
    out_3[1] = total[4:6]

    pltpu.make_async_copy(best, best, send_sem.at[0]).wait()
    pltpu.make_async_copy(merged, merged, send_sem.at[1]).wait()
    to_partner.wait_send()

    @pl.when(has_target)
    def _():
        to_target.wait_send()


def write_out(*refs):
    count = len(refs) // 2
    semaphores = refs[-1]
    copies = [pltpu.make_async_copy(refs[n], refs[count + n], semaphores.at[n]) for n in range(count)]
    for copy in copies:
        copy.start()
    for copy in copies:
        copy.wait()


def body(red_band, nir_band, cloud_class, date_ordinal):
    dates, strip, width = red_band.shape
    own = strip // 2
    chunk = strip // 4
    half = width // 2
    whole = pl.BlockSpec(memory_space=pltpu.VMEM)
    anywhere = pl.BlockSpec(memory_space=pl.ANY)
    outs = [jax.ShapeDtypeStruct((own, width), jnp.int32)] * 3
    outs += [jax.ShapeDtypeStruct((2, own >> n, width >> n), jnp.float32) for n in range(1, LEVELS + 1)]
    kept = [pltpu.VMEM(out.shape, out.dtype) for out in outs]
    pieces = [(0, start, half // 2) for start in range(0, width, half // 2)]
    pieces += [(slot, start, half) for slot in range(1, 4) for start in (0, half)]
    table = row_weights(own)

    def run(*refs):
        kernel(*refs, pieces=pieces)

    results = pl.pallas_call(
        run,
        out_shape=kept,
        in_specs=[anywhere] * 5,
        out_specs=[whole] * 6,
        scratch_shapes=[
            pltpu.VMEM((4, 3, dates, chunk, width), jnp.int32),
            pltpu.VMEM((2, 3, chunk, width), jnp.int32),
            pltpu.VMEM((2, 3, chunk, width), jnp.int32),
            pltpu.VMEM((2, 3, chunk, width), jnp.int32),
            pltpu.VMEM((8 * chunk, width + 2 * LANES), jnp.bfloat16),
            pltpu.VMEM((8 * chunk, width // 2 + 2 * LANES), jnp.bfloat16),
            pltpu.VMEM((8 * chunk, width // 4 + 2 * LANES), jnp.bfloat16),
            pltpu.VMEM((2, TILE, half), jnp.float32),
            pltpu.VMEM((TILE, half), jnp.float32),
            pltpu.VMEM((3 * TILE, half), jnp.float32),
            pltpu.VMEM((3 * TILE, half), jnp.float32),
            pltpu.VMEM(table.shape[1:], jnp.bfloat16),
            pltpu.SMEM((dates,), jnp.int32),
            pltpu.SemaphoreType.DMA((len(pieces),)),
            pltpu.SemaphoreType.DMA((2,)),
            pltpu.SemaphoreType.DMA((4,)),
            pltpu.SemaphoreType.DMA((2, 2)),
            pltpu.SemaphoreType.DMA((3,)),
        ],
        compiler_params=pltpu.CompilerParams(collective_id=0, has_side_effects=True),
        name="composite",
    )(red_band, nir_band, cloud_class, date_ordinal, jnp.asarray(table))
    return pl.pallas_call(
        write_out,
        out_shape=outs,
        in_specs=[whole] * 6,
        out_specs=[anywhere] * 6,
        scratch_shapes=[pltpu.SemaphoreType.DMA((6,))],
        name="write_out",
    )(*[pltpu.with_memory_space_constraint(result, pltpu.VMEM) for result in results])


def solution(mesh):
    in_specs = (
        P("dates", ("tiles", "rows"), None),
        P("dates", ("tiles", "rows"), None),
        P("dates", ("tiles", "rows"), None),
        P(("tiles", "dates")),
    )
    out_specs = (
        P(("tiles", "rows", "dates"), None),
        P(("tiles", "rows", "dates"), None),
        P(("tiles", "rows", "dates"), None),
        P(None, ("tiles", "rows", "dates"), None),
        P(None, ("tiles", "rows", "dates"), None),
        P(None, ("tiles", "rows", "dates"), None),
    )
    return jax.shard_map(body, mesh=mesh, in_specs=in_specs, out_specs=out_specs, check_vma=False)
```

```python
import jax
import jax.numpy as jnp
import numpy as np
from jax import lax
from jax.experimental import pallas as pl
from jax.experimental.pallas import tpu as pltpu
from jax.sharding import PartitionSpec as P

LEVELS = 3
LIMB_BITS = 15
LIMB_MASK = (1 << LIMB_BITS) - 1
FLAG = 1 << 30
SCALE_BAND = 2.0**-30
LANES = 128
TILE = 8
WIDTH = 512
AT_2, AT_3 = 3, 71
MESH = pl.DeviceIdType.MESH
TAPS = np.array([1, 5, 10, 10, 5, 1], np.float64) / 32


def tap(distance):
    return TAPS[distance] if 0 <= distance < len(TAPS) else 0.0


def limbs(value):
    return value >> LIMB_BITS, value & LIMB_MASK


def take_first(first, second):
    r1a, r0a, n1a, n0a, clear_a, ord_a = first
    r1b, r0b, n1b, n0b, clear_b, ord_b = second
    low = n0a * r0b - n0b * r0a + ((ord_b - ord_a) >> 31)
    mid = (n1a * r0b + n0a * r1b) - (n1b * r0a + n0b * r1a) + (low >> LIMB_BITS)
    high = n1a * r1b - n1b * r1a + (mid >> LIMB_BITS)
    return high >= clear_b - clear_a


def pick(take, first, second):
    return tuple(jnp.where(take, one, two) for one, two in zip(first, second))


def joined(entry):
    r1, r0, n1, n0, clear, order = entry
    return (r1 << LIMB_BITS) | r0, (n1 << LIMB_BITS) | n0, clear, order


def split(value):
    high = value.astype(jnp.bfloat16)
    return high, (value - high.astype(jnp.float32)).astype(jnp.bfloat16)


def iota(shape, axis):
    return lax.broadcasted_iota(jnp.int32, shape, axis)


def column_weights():
    columns = range(2 * LANES)
    one = {j: np.array([tap(c - 2 * j + 2) for c in columns]) for j in range(-12, LANES + 12)}
    two = {i: sum(TAPS[d] * one[2 * i - 2 + d] for d in range(6)) for i in range(-5, LANES // 2 + 5)}
    three = {p: sum(TAPS[d] * two[2 * p - 2 + d] for d in range(6)) for p in range(-1, LANES // 4 + 1)}
    three[-2] = sum(TAPS[d] * two[-6 + d] for d in range(1, 6))
    three[LANES // 4 + 1] = sum(TAPS[d] * two[LANES // 2 + d] for d in range(5))
    table = np.zeros((2 * LANES, 3 * LANES))
    for j in range(LANES):
        table[:, j] = one[j]
    table[:, LANES] = one[LANES]
    table[:, 2 * LANES - 1] = one[-1]
    for i in range(-2, LANES // 2 + 2):
        table[:, LANES + AT_2 + i] = two[i]
    for p in range(-2, LANES // 4 + 2):
        top = three[p].astype(jnp.bfloat16).astype(np.float64)
        table[:, LANES + AT_3 + p] = top
        table[:, 2 * LANES + AT_3 + p] = three[p] - top
    return table.astype(jnp.bfloat16)


def row_weights(own):
    chunk = own // 2
    table = np.zeros((4, 8 * TILE, LANES))
    for side in range(2):
        for outer in range(2):

            def level_row(level, row):
                if level == 0:
                    return np.eye(own)[row] if 0 <= row < own else np.zeros(own)
                beyond = row < 0 if side == 0 else row >= own >> level
                if beyond and not outer:
                    return np.zeros(own)
                return sum(TAPS[d] * level_row(level - 1, 2 * row - 2 + d) for d in range(6))

            def put(m, band, level, row, second=None):
                weights = level_row(level, row) * SCALE_BAND
                for k in range(4 * own):
                    if (k // chunk) % 2 != band:
                        continue
                    place = (k // own) % 2
                    place = place if side == 0 else 1 - place
                    value = weights[place * chunk + k % chunk]
                    top = np.float64(np.asarray(value, jnp.bfloat16))
                    table[2 * side + outer, m, k] = top
                    if second is not None:
                        table[2 * side + outer, second, k] = value - top

            for band in range(2):
                for beside in range(2):
                    ends = [(-1,), (-2, -1), (-2, -1)]
                    low = (beside == 0) == (side == 0)
                    rows = [[row if low else (own >> level + 1) - 1 - row for row in ends[level]] for level in range(LEVELS)]
                    rows = [sorted(some) for some in rows]
                    put(beside * TILE + 4 + band, band, 1, rows[0][0])
                    for n in range(2):
                        put(beside * TILE + 2 * band + n, band, 2, rows[1][n])
                        m = 4 * beside + 2 * band + n
                        put(2 * TILE + m, band, 3, rows[2][n], 7 * TILE + m)
                for row in range(own // 4):
                    put(3 * TILE + band * (own // 4) + row, band, 2, row)
                for row in range(own // 2):
                    put(4 * TILE + band * (own // 2) + row, band, 1, row)
                for row in range(own // 8):
                    m = band * (own // 8) + row
                    put(6 * TILE + m, band, 3, row, 6 * TILE + 4 + m)
    return table.astype(jnp.bfloat16)


def kernel(
    red, nir, cloud, ordinals, row_table, column_table, out_red, out_nir, out_ord, out_1, out_2, out_3,
    stream, best, arrived, merged, parts, message, received, home, homed, third, weights, columns_by,
    ords, load_sem, order_sem, send_sem, best_sem, sum_sem, pieces,
):
    tile = lax.axis_index("tiles")
    strip_index = lax.axis_index("rows")
    core = lax.axis_index("dates")
    strips = lax.axis_size("rows")
    dates, strip, width = red.shape
    chunk = strip // 4
    half = width // 2
    toward = 1 - 2 * core
    has_target = jnp.where(core == 0, strip_index < strips - 1, strip_index > 0)
    has_source = jnp.where(core == 0, strip_index > 0, strip_index < strips - 1)
    partner = (tile, strip_index, 1 - core)
    target = (tile, jnp.clip(strip_index + toward, 0, strips - 1), core)
    source_device = (tile, jnp.clip(strip_index - toward, 0, strips - 1), core)
    rows_of = [3 * core * chunk, (1 + core) * chunk, (3 - 3 * core) * chunk, (2 - core) * chunk]

    arrivals = []
    for number, (slot, start, size) in enumerate(pieces):
        begin = pl.multiple_of(rows_of[slot], chunk)
        columns = pl.ds(start, size)
        for band, source in enumerate((red, nir, cloud)):
            pltpu.make_async_copy(
                source.at[:, pl.ds(begin, chunk), columns],
                stream.at[slot, band, :, :, columns],
                load_sem.at[number],
            ).start()
        whole = stream.at[slot, :, :, :, columns]
        arrivals.append(pltpu.make_async_copy(whole, whole, load_sem.at[number]))
    order_copy = pltpu.make_async_copy(ordinals, ords, order_sem.at[0])
    order_copy.start()
    case = 2 * (1 - core) + has_target.astype(jnp.int32)
    table_copies = [
        pltpu.make_async_copy(row_table.at[case], weights, order_sem.at[1]),
        pltpu.make_async_copy(column_table, columns_by, order_sem.at[2]),
    ]
    for copy in table_copies:
        copy.start()

    barrier = pltpu.get_barrier_semaphore()
    pl.semaphore_signal(barrier, inc=1, device_id=partner, device_id_type=MESH)

    @pl.when(has_source)
    def _():
        pl.semaphore_signal(barrier, inc=1, device_id=source_device, device_id_type=MESH)

    @pl.when(jnp.logical_not(has_source))
    def _():
        received[...] = jnp.zeros(received.shape, jnp.float32)

    order_copy.wait()

    def find_best(slot, start, size, own):
        place = slot - 2

        def step(number, unused):
            at = pl.multiple_of(number * WIDTH + start, WIDTH)
            columns = pl.ds(at, WIDTH)

            def entry(date):
                red_hi, red_lo = limbs(stream[slot, 0, date, :, columns])
                nir_hi, nir_lo = limbs(stream[slot, 1, date, :, columns])
                clear = jnp.where(stream[slot, 2, date, :, columns] == 0, FLAG, 0)
                return (red_hi, red_lo, nir_hi, nir_lo, clear, ords[date])

            current = None
            if own:
                red_hi, red_lo = limbs(arrived[place, 0, :, columns])
                nir_hi, nir_lo = limbs(arrived[place, 1, :, columns])
                packed = arrived[place, 2, :, columns]
                current = (red_hi, red_lo, nir_hi, nir_lo, packed & FLAG, packed & (FLAG - 1))
            for date in range(0, dates, 2):
                other = entry(date)
                if date + 1 < dates:
                    later = entry(date + 1)
                    other = pick(take_first(later, other), later, other)
                current = other if current is None else pick(take_first(other, current), other, current)
            value_red, value_nir, clear, order = joined(current)
            if own:
                merged[place, 0, :, columns] = value_red
                merged[place, 1, :, columns] = value_nir
                merged[place, 2, :, columns] = order
                both = jnp.concatenate([value_red, value_nir], axis=0).astype(jnp.float32)
                high, low = split(both)
                parts[0, place * 2 * chunk : (place + 1) * 2 * chunk, columns] = high
                parts[1, place * 2 * chunk : (place + 1) * 2 * chunk, columns] = low
            else:
                best[slot, 0, :, columns] = value_red
                best[slot, 1, :, columns] = value_nir
                best[slot, 2, :, columns] = clear + order
            return unused

        lax.fori_loop(0, size // WIDTH, step, 0)

    def best_copy(slot, part):
        columns = pl.ds(part * half, half)
        return pltpu.make_async_remote_copy(
            src_ref=best.at[slot, :, :, columns],
            dst_ref=arrived.at[slot, :, :, columns],
            send_sem=send_sem.at[0],
            recv_sem=best_sem.at[slot, part],
            device_id=partner,
            device_id_type=MESH,
        )

    waiting = list(zip(pieces, arrivals))

    def run(slot, part):
        begin, end = part * half, (part + 1) * half
        at = begin
        while at < end:
            if waiting and waiting[0][0][:2] == (slot, at):
                waiting.pop(0)[1].wait()
            stop = min([end] + [piece[1] for piece, _ in waiting if piece[0] == slot and piece[1] > at])
            find_best(slot, at, stop - at, slot >= 2)
            at = stop

    for slot in range(2):
        for part in range(2):
            run(slot, part)
            if slot == 0 and part == 0:
                pl.semaphore_wait(barrier, 1 + has_target.astype(jnp.int32))
            best_copy(slot, part).start()
    for slot in range(2):
        for part in range(2):
            best_copy(slot, part).wait_recv()
            run(slot + 2, part)
        merged_rows = pl.ds(pl.multiple_of(((1 - core) if slot == 0 else core) * chunk, chunk), chunk)
        for number, result in enumerate((out_red, out_nir, out_ord)):
            pltpu.make_async_remote_copy(
                src_ref=merged.at[slot, number],
                dst_ref=result.at[merged_rows],
                send_sem=send_sem.at[1],
                recv_sem=sum_sem.at[0],
                device_id=partner,
                device_id_type=MESH,
            ).start()
    for copy in table_copies:
        copy.wait()

    block = 2 * LANES
    blocks = width // block
    count = 4 * chunk

    def stacked(part):
        return jnp.concatenate([parts[part, :, b * block : (b + 1) * block] for b in range(blocks)], axis=0)

    def product(left, right):
        return jnp.dot(left, right, preferred_element_type=jnp.float32)

    high, low = stacked(0), stacked(1)
    first = columns_by[:, 0:block]
    shares = product(high, first) + product(low, first)
    second = product(high, columns_by[:, block : block + LANES])
    data = []
    for b in range(blocks):
        rows = slice(b * count, (b + 1) * count)
        for value in (shares[rows, 0:LANES], shares[rows, LANES:] + second[rows]):
            data.append(jnp.concatenate(split(value), axis=0))
    sums = product(weights[:, 0 : 2 * count], jnp.concatenate(data, axis=1))
    lane = iota((TILE, LANES), 1)

    def tile_of(number, b, half_of):
        at = b * block + half_of * LANES
        return sums[number * TILE : (number + 1) * TILE, at : at + LANES]

    def rolled(value, shift):
        return pltpu.roll(value, shift % LANES, 1)

    def only(mask, value):
        return jnp.where(mask, value, 0.0)

    def level_1(number):
        tiles = []
        for b in range(blocks):
            value = tile_of(number, b, 0)
            if b > 0:
                value = value + only(lane == 0, tile_of(number, b - 1, 1))
            if b + 1 < blocks:
                value = value + only(lane == LANES - 1, tile_of(number, b + 1, 1))
            tiles.append(value)
        return tiles

    def gathered(shares_of, at, per):
        size = LANES // per
        tiles = [None] * (blocks // per)

        def put(number, value):
            if 0 <= number < len(tiles):
                tiles[number] = value if tiles[number] is None else tiles[number] + value

        for b in range(blocks):
            number, start = b // per, (b % per) * size
            value = rolled(shares_of[b], start - at)
            put(number, only((lane >= start - 2) & (lane < start + size + 2), value))
            if b % per == 0:
                put(number - 1, only(lane >= LANES - 2, value))
            if b % per == per - 1:
                put(number + 1, only(lane < 2, value))
        return tiles

    def level_2(number):
        shares_of = [tile_of(number, b, 1) for b in range(blocks)]
        tiles = gathered(shares_of, AT_2, 2)
        left, right = shares_of[0], shares_of[-1]
        tiles[0] = tiles[0] - only(lane == 0, rolled(left, 1) * TAPS[1])
        tiles[-1] = tiles[-1] - only(lane == LANES - 1, rolled(right, -1) * TAPS[4])
        return tiles

    def level_3(shares_of):
        tiles = gathered(shares_of, AT_3, 4)
        left, right = shares_of[0], shares_of[-1]
        edge = rolled(left, 2 - AT_2) * TAPS[0] + rolled(left, 1 - AT_2) * TAPS[1] + rolled(left, 1) * (TAPS[2] * TAPS[1])
        next_edge = rolled(left, 2) * (TAPS[0] * TAPS[1])
        tiles[0] = tiles[0] - only(lane == 0, edge) - only(lane == 1, next_edge)
        beyond = AT_2 + LANES // 2
        edge = rolled(right, -1 - beyond) * TAPS[4] + rolled(right, -2 - beyond) * TAPS[5]
        edge = edge + rolled(right, -1) * (TAPS[3] * TAPS[4])
        next_edge = rolled(right, -2) * (TAPS[5] * TAPS[4])
        tiles[-1] = tiles[-1] - only(lane == LANES - 1, edge) - only(lane == LANES - 2, next_edge)
        return tiles

    ends = (half // 2, half // 2 + half // 4)
    row = iota((TILE, LANES), 0)

    def fill(held, one, two, three):
        for number, value in enumerate(one):
            if number < len(two) + len(three):
                value = jnp.where(row < 4, (two + three)[number], value)
            held[:, number * LANES : (number + 1) * LANES] = value

    ends_3 = level_3([tile_of(2, b, 1) + tile_of(7, b, 1) for b in range(blocks)])
    to_target = pltpu.make_async_remote_copy(
        src_ref=message.at[0],
        dst_ref=received,
        send_sem=send_sem.at[2],
        recv_sem=sum_sem.at[1],
        device_id=target,
        device_id_type=MESH,
    )
    to_partner = pltpu.make_async_remote_copy(
        src_ref=home,
        dst_ref=homed,
        send_sem=send_sem.at[3],
        recv_sem=sum_sem.at[2],
        device_id=partner,
        device_id_type=MESH,
    )
    fill(message.at[0], level_1(0), level_2(0), ends_3)

    @pl.when(has_target)
    def _():
        to_target.start()

    own_3 = level_3([tile_of(6, b, 1) for b in range(blocks)])
    for band in range(2):
        for number, value in enumerate(level_1(4 + band)):
            home[band * TILE : (band + 1) * TILE, number * LANES : (number + 1) * LANES] = value
    unused = [jnp.zeros((TILE, LANES), jnp.float32)] * 2
    for number, value in enumerate(level_2(3) + own_3 + unused):
        home[2 * TILE :, number * LANES : (number + 1) * LANES] = value
    to_partner.start()
    fill(message.at[1], level_1(1), level_2(1), [])
    for number, value in enumerate(ends_3):
        third[:, number * LANES : (number + 1) * LANES] = value
    to_partner.wait_recv()
    pltpu.make_async_copy(merged, merged, sum_sem.at[0]).wait()

    @pl.when(has_source)
    def _():
        to_target.wait_recv()

    sides = (received, message.at[1])

    def spread(side, row, columns):
        return jnp.broadcast_to(sides[side][row : row + 1, columns], (TILE, columns.stop - columns.start))

    row = iota((TILE, half), 0)
    edges = ((TILE - 1) * core, (TILE - 1) * (1 - core))
    for band in range(2):
        total = homed[band * TILE : (band + 1) * TILE]
        for side in range(2):
            total = total + jnp.where(row == edges[side], spread(side, 4 + band, slice(0, half)), 0.0)
        out_1[band] = total
    row = iota((TILE, ends[0]), 0)
    total = homed[2 * TILE :, 0 : ends[0]]
    for side in range(2):
        shift = 2 * (core if side == 0 else 1 - core)
        for number in range(4):
            target = number % 2 + 4 * (number // 2) + shift
            total = total + jnp.where(row == target, spread(side, number, slice(0, ends[0])), 0.0)
    out_2[0] = total[0:4]
    out_2[1] = total[4:8]
    last = slice(ends[0], ends[1])
    total = homed[2 * TILE : 2 * TILE + 4, last] + homed[2 * TILE + 4 :, last] + received[0:4, last] + third[4:8]
    out_3[0] = total[0:2]
    out_3[1] = total[2:4]

    pltpu.make_async_copy(best, best, send_sem.at[0]).wait()
    pltpu.make_async_copy(merged, merged, send_sem.at[1]).wait()
    to_partner.wait_send()

    @pl.when(has_target)
    def _():
        to_target.wait_send()


def write_out(*refs):
    count = len(refs) // 2
    semaphores = refs[-1]
    copies = [pltpu.make_async_copy(refs[n], refs[count + n], semaphores.at[n]) for n in range(count)]
    for copy in copies:
        copy.start()
    for copy in copies:
        copy.wait()


def body(red_band, nir_band, cloud_class, date_ordinal):
    dates, strip, width = red_band.shape
    own = strip // 2
    chunk = strip // 4
    half = width // 2
    whole = pl.BlockSpec(memory_space=pltpu.VMEM)
    anywhere = pl.BlockSpec(memory_space=pl.ANY)
    outs = [jax.ShapeDtypeStruct((own, width), jnp.int32)] * 3
    outs += [jax.ShapeDtypeStruct((2, own >> n, width >> n), jnp.float32) for n in range(1, LEVELS + 1)]
    kept = [pltpu.VMEM(out.shape, out.dtype) for out in outs]
    pieces = [(0, start, half // 2) for start in range(0, width, half // 2)]
    pieces += [(slot, start, half) for slot in range(1, 4) for start in (0, half)]
    row_table, column_table = row_weights(own), column_weights()

    def run(*refs):
        kernel(*refs, pieces=pieces)

    results = pl.pallas_call(
        run,
        out_shape=kept,
        in_specs=[anywhere] * 6,
        out_specs=[whole] * 6,
        scratch_shapes=[
            pltpu.VMEM((4, 3, dates, chunk, width), jnp.int32),
            pltpu.VMEM((2, 3, chunk, width), jnp.int32),
            pltpu.VMEM((2, 3, chunk, width), jnp.int32),
            pltpu.VMEM((2, 3, chunk, width), jnp.int32),
            pltpu.VMEM((2, 4 * chunk, width), jnp.bfloat16),
            pltpu.VMEM((2, TILE, half), jnp.float32),
            pltpu.VMEM((TILE, half), jnp.float32),
            pltpu.VMEM((3 * TILE, half), jnp.float32),
            pltpu.VMEM((3 * TILE, half), jnp.float32),
            pltpu.VMEM((TILE, half // 4), jnp.float32),
            pltpu.VMEM(row_table.shape[1:], jnp.bfloat16),
            pltpu.VMEM(column_table.shape, jnp.bfloat16),
            pltpu.SMEM((dates,), jnp.int32),
            pltpu.SemaphoreType.DMA((len(pieces),)),
            pltpu.SemaphoreType.DMA((3,)),
            pltpu.SemaphoreType.DMA((4,)),
            pltpu.SemaphoreType.DMA((2, 2)),
            pltpu.SemaphoreType.DMA((3,)),
        ],
        compiler_params=pltpu.CompilerParams(collective_id=0, has_side_effects=True),
        name="composite",
    )(red_band, nir_band, cloud_class, date_ordinal, jnp.asarray(row_table), jnp.asarray(column_table))
    return pl.pallas_call(
        write_out,
        out_shape=outs,
        in_specs=[whole] * 6,
        out_specs=[anywhere] * 6,
        scratch_shapes=[pltpu.SemaphoreType.DMA((6,))],
        name="write_out",
    )(*[pltpu.with_memory_space_constraint(result, pltpu.VMEM) for result in results])


def solution(mesh):
    in_specs = (
        P("dates", ("tiles", "rows"), None),
        P("dates", ("tiles", "rows"), None),
        P("dates", ("tiles", "rows"), None),
        P(("tiles", "dates")),
    )
    out_specs = (
        P(("tiles", "rows", "dates"), None),
        P(("tiles", "rows", "dates"), None),
        P(("tiles", "rows", "dates"), None),
        P(None, ("tiles", "rows", "dates"), None),
        P(None, ("tiles", "rows", "dates"), None),
        P(None, ("tiles", "rows", "dates"), None),
    )
    return jax.shard_map(body, mesh=mesh, in_specs=in_specs, out_specs=out_specs, check_vma=False)
```

```python
import jax
import jax.numpy as jnp
import numpy as np
from jax import lax
from jax.experimental import pallas as pl
from jax.experimental.pallas import tpu as pltpu
from jax.sharding import PartitionSpec as P

LEVELS = 3
LIMB_BITS = 15
LIMB_MASK = (1 << LIMB_BITS) - 1
FLAG = 1 << 30
SCALE_BAND = 2.0**-30
LANES = 128
TILE = 8
WIDTH = 512
AT_2, AT_3 = 3, 71
SENT = 6
PIECES = ((0,512),(512,512),(1024,512),(1536,512))
MESH = pl.DeviceIdType.MESH
TAPS = np.array([1, 5, 10, 10, 5, 1], np.float64) / 32


def tap(distance):
    return TAPS[distance] if 0 <= distance < len(TAPS) else 0.0


def limbs(value):
    return value >> LIMB_BITS, value & LIMB_MASK


def take_first(first, second, earlier):
    r1a, r0a, n1a, n0a, clear_a, ord_a = first
    r1b, r0b, n1b, n0b, clear_b, ord_b = second
    low = n0a * r0b - n0b * r0a
    if not earlier:
        low = low + ((ord_b - ord_a) >> 31)
    mid = (n1a * r0b + n0a * r1b) - (n1b * r0a + n0b * r1a) + (low >> LIMB_BITS)
    high = n1a * r1b - n1b * r1a + (mid >> LIMB_BITS)
    return high >= clear_b - clear_a


def pick(take, first, second):
    return tuple(jnp.where(take, one, two) for one, two in zip(first, second))


def sorted_scalars(keys):
    keys, count = list(keys), len(keys)
    top = 1
    while 2 * top < count:
        top *= 2
    p = top
    while p:
        q, r, d = top, 0, p
        while True:
            for i in range(count - d):
                if i & p == r:
                    low, high = keys[i], keys[i + d]
                    keys[i], keys[i + d] = jnp.minimum(low, high), jnp.maximum(low, high)
            if q == p:
                break
            d, q, r = q - p, q // 2, p
        p //= 2
    return keys


def joined(entry):
    r1, r0, n1, n0, clear, order = entry
    return (r1 << LIMB_BITS) | r0, (n1 << LIMB_BITS) | n0, clear, order


def split(value):
    high = value.astype(jnp.bfloat16)
    return high, (value - high.astype(jnp.float32)).astype(jnp.bfloat16)


def iota(shape, axis):
    return lax.broadcasted_iota(jnp.int32, shape, axis)


def column_weights():
    columns = range(2 * LANES)
    one = {j: np.array([tap(c - 2 * j + 2) for c in columns]) for j in range(-12, LANES + 12)}
    two = {i: sum(TAPS[d] * one[2 * i - 2 + d] for d in range(6)) for i in range(-5, LANES // 2 + 5)}
    three = {p: sum(TAPS[d] * two[2 * p - 2 + d] for d in range(6)) for p in range(-1, LANES // 4 + 1)}
    three[-2] = sum(TAPS[d] * two[-6 + d] for d in range(1, 6))
    three[LANES // 4 + 1] = sum(TAPS[d] * two[LANES // 2 + d] for d in range(5))
    table = np.zeros((2 * LANES, 3 * LANES))
    for j in range(LANES):
        table[:, j] = one[j]
    table[:, LANES] = one[LANES]
    table[:, 2 * LANES - 1] = one[-1]
    for i in range(-2, LANES // 2 + 2):
        table[:, LANES + AT_2 + i] = two[i]
    for p in range(-2, LANES // 4 + 2):
        top = three[p].astype(jnp.bfloat16).astype(np.float64)
        table[:, LANES + AT_3 + p] = top
        table[:, 2 * LANES + AT_3 + p] = three[p] - top
    return table.astype(jnp.bfloat16)


def row_weights(own):
    chunk = own // 2
    table = np.zeros((4, 8 * TILE, LANES))
    for side in range(2):
        for outer in range(2):

            def level_row(level, row):
                if level == 0:
                    return np.eye(own)[row] if 0 <= row < own else np.zeros(own)
                beyond = row < 0 if side == 0 else row >= own >> level
                if beyond and not outer:
                    return np.zeros(own)
                return sum(TAPS[d] * level_row(level - 1, 2 * row - 2 + d) for d in range(6))

            def put(m, band, level, row, second=None):
                weights = level_row(level, row) * SCALE_BAND
                for k in range(4 * own):
                    if (k // chunk) % 2 != band:
                        continue
                    place = (k // own) % 2
                    place = place if side == 0 else 1 - place
                    value = weights[place * chunk + k % chunk]
                    top = np.float64(np.asarray(value, jnp.bfloat16))
                    table[2 * side + outer, m, k] = top
                    if second is not None:
                        table[2 * side + outer, second, k] = value - top

            for band in range(2):
                for beside in range(2):
                    ends = [(-1,), (-2, -1), (-2, -1)]
                    low = (beside == 0) == (side == 0)
                    rows = [[row if low else (own >> level + 1) - 1 - row for row in ends[level]] for level in range(LEVELS)]
                    rows = [sorted(some) for some in rows]
                    put(beside * TILE + 4 + band, band, 1, rows[0][0])
                    for n in range(2):
                        put(beside * TILE + 2 * band + n, band, 2, rows[1][n])
                        m = 4 * beside + 2 * band + n
                        put(2 * TILE + m, band, 3, rows[2][n], 7 * TILE + m)
                for row in range(own // 4):
                    put(3 * TILE + band * (own // 4) + row, band, 2, row)
                for row in range(own // 2):
                    put(4 * TILE + band * (own // 2) + row, band, 1, row)
                for row in range(own // 8):
                    m = band * (own // 8) + row
                    put(6 * TILE + m, band, 3, row, 6 * TILE + 4 + m)
    return table.astype(jnp.bfloat16)


def kernel(
    red, nir, cloud, ordinals, table, out_red, out_nir, out_ord, out_1, out_2, out_3,
    best, arrived, parts, message, outbox, beside, received, homed, third, weights,
    ords, turns, load_sem, order_sem, send_sem, best_sem, sum_sem, *streams, pieces,
):
    tile = lax.axis_index("tiles")
    strip_index = lax.axis_index("rows")
    core = lax.axis_index("dates")
    strips = lax.axis_size("rows")
    dates, strip, width = red.shape
    chunk = strip // 4
    half = width // 2
    toward = 1 - 2 * core
    has_target = jnp.where(core == 0, strip_index < strips - 1, strip_index > 0)
    has_source = jnp.where(core == 0, strip_index > 0, strip_index < strips - 1)
    partner = (tile, strip_index, 1 - core)
    target = (tile, jnp.clip(strip_index + toward, 0, strips - 1), core)
    source_device = (tile, jnp.clip(strip_index - toward, 0, strips - 1), core)
    rows_of = [3 * core * chunk, (1 + core) * chunk, (3 - 3 * core) * chunk, (2 - core) * chunk]

    arrivals = []

    def start_load(number):
        slot, start, size = pieces[number]
        semaphore = load_sem.at[number % load_sem.shape[0]]
        begin = pl.multiple_of(rows_of[slot], chunk)
        columns = pl.ds(start, size)
        for band, source in enumerate((red, nir, cloud)):
            pltpu.make_async_copy(
                source.at[:, pl.ds(begin, chunk), columns],
                streams[number].at[band],
                semaphore,
            ).start()
        arrivals.append(pltpu.make_async_copy(streams[number], streams[number], semaphore))

    def wait_load(number):
        arrivals[number].wait()
        if len(arrivals) < len(pieces):
            start_load(len(arrivals))

    for number in range(load_sem.shape[0]):
        start_load(number)
    order_copy = pltpu.make_async_copy(ordinals, ords, order_sem.at[0])
    order_copy.start()
    case = 2 * (1 - core) + has_target.astype(jnp.int32)
    table_copy = pltpu.make_async_copy(table.at[case], weights, order_sem.at[1])
    table_copy.start()

    barrier = pltpu.get_barrier_semaphore()
    pl.semaphore_signal(barrier, inc=1, device_id=partner, device_id_type=MESH)

    @pl.when(has_source)
    def _():
        pl.semaphore_signal(barrier, inc=1, device_id=source_device, device_id_type=MESH)

    @pl.when(jnp.logical_not(has_source))
    def _():
        received[...] = jnp.zeros(received.shape, jnp.float32)

    order_copy.wait()
    for number, key in enumerate(sorted_scalars([ords[date] * dates + date for date in range(dates)])):
        turns[0, number] = key % dates
        turns[1, number] = key // dates

    def find_best(slot, start, size, own, stream, origin):
        place = slot - 2
        wide = min(size, WIDTH)

        def step(number, unused):
            at = pl.multiple_of(number * wide + start, wide)
            columns = pl.ds(at, wide)
            held = pl.ds(pl.multiple_of(at - origin, wide), wide)

            def entry(turn):
                date = turns[0, turn]
                red_hi, red_lo = limbs(stream[0, date, :, held])
                nir_hi, nir_lo = limbs(stream[1, date, :, held])
                clear = jnp.where(stream[2, date, :, held] == 0, FLAG, 0)
                return (red_hi, red_lo, nir_hi, nir_lo, clear, turns[1, turn])

            def first_of(one, two, earlier):
                return pick(take_first(one, two, earlier), one, two)

            current = None
            for turn in range(0, dates, 2):
                other = entry(turn)
                if turn + 1 < dates:
                    other = first_of(other, entry(turn + 1), True)
                current = other if current is None else first_of(current, other, True)
            if own:
                red_hi, red_lo = limbs(arrived[place, 0, :, columns])
                nir_hi, nir_lo = limbs(arrived[place, 1, :, columns])
                packed = arrived[place, 2, :, columns]
                theirs = (red_hi, red_lo, nir_hi, nir_lo, packed & FLAG, packed & (FLAG - 1))
                current = first_of(theirs, current, False)
            value_red, value_nir, clear, order = joined(current)
            if own:
                best[slot, 0, :, columns] = value_red
                best[slot, 1, :, columns] = value_nir
                best[slot, 2, :, columns] = order
                both = jnp.concatenate([value_red, value_nir], axis=0).astype(jnp.float32)
                high, low = split(both)
                parts[0, place * 2 * chunk : (place + 1) * 2 * chunk, columns] = high
                parts[1, place * 2 * chunk : (place + 1) * 2 * chunk, columns] = low
            else:
                best[slot, 0, :, columns] = value_red
                best[slot, 1, :, columns] = value_nir
                best[slot, 2, :, columns] = clear + order
            return unused

        lax.fori_loop(0, size // wide, step, 0, unroll=True)

    def best_copy(slot, part):
        columns = pl.ds(part * half, half)
        return pltpu.make_async_remote_copy(
            src_ref=best.at[slot, :, :, columns],
            dst_ref=arrived.at[slot, :, :, columns],
            send_sem=send_sem.at[0],
            recv_sem=best_sem.at[slot, part],
            device_id=partner,
            device_id_type=MESH,
        )

    waiting = list(enumerate(pieces))

    def run(slot, part):
        begin, end = part * half, (part + 1) * half
        at = begin
        while at < end:
            if waiting and waiting[0][1][:2] == (slot, at):
                wait_load(waiting.pop(0)[0])
            stop = min([end] + [piece[1] for _, piece in waiting if piece[0] == slot and piece[1] > at])
            holder = max(n for n, piece in enumerate(pieces) if piece[0] == slot and piece[1] <= at)
            find_best(slot, at, stop - at, slot >= 2, streams[holder], pieces[holder][1])
            at = stop

    for slot in range(2):
        for part in range(2):
            run(slot, part)
            if slot == 0 and part == 0:
                pl.semaphore_wait(barrier, 1 + has_target.astype(jnp.int32))
            best_copy(slot, part).start()
    for slot in range(2):
        for part in range(2):
            best_copy(slot, part).wait_recv()
            run(slot + 2, part)
        merged_rows = pl.ds(pl.multiple_of(((1 - core) if slot == 0 else core) * chunk, chunk), chunk)
        for number, result in enumerate((out_red, out_nir, out_ord)):
            pltpu.make_async_remote_copy(
                src_ref=best.at[slot + 2, number],
                dst_ref=result.at[merged_rows],
                send_sem=send_sem.at[0],
                recv_sem=sum_sem.at[0],
                device_id=partner,
                device_id_type=MESH,
            ).start()
    table_copy.wait()

    block = 2 * LANES
    blocks = width // block
    count = 4 * chunk

    def stacked(part):
        return jnp.concatenate([parts[part, :, b * block : (b + 1) * block] for b in range(blocks)], axis=0)

    def product(left, right):
        return jnp.dot(left, right, preferred_element_type=jnp.float32)

    high, low = stacked(0), stacked(1)
    base = 8 * TILE
    first = jnp.concatenate([weights[base : base + block], weights[base + block : base + 2 * block]], axis=1)
    shares = product(high, first) + product(low, first)
    second = product(high, weights[base + 2 * block : base + 3 * block])
    data = []
    for b in range(blocks):
        rows = slice(b * count, (b + 1) * count)
        for value in (shares[rows, 0:LANES], shares[rows, LANES:] + second[rows]):
            data.append(jnp.concatenate(split(value), axis=0))
    sums = product(weights[0:base, 0 : 2 * count], jnp.concatenate(data, axis=1))
    lane = iota((TILE, LANES), 1)

    def tile_of(number, b, half_of):
        at = b * block + half_of * LANES
        return sums[number * TILE : (number + 1) * TILE, at : at + LANES]

    def rolled(value, shift):
        return pltpu.roll(value, shift % LANES, 1)

    def only(mask, value):
        return jnp.where(mask, value, 0.0)

    def level_1(number):
        tiles = []
        for b in range(blocks):
            value = tile_of(number, b, 0)
            if b > 0:
                value = value + only(lane == 0, tile_of(number, b - 1, 1))
            if b + 1 < blocks:
                value = value + only(lane == LANES - 1, tile_of(number, b + 1, 1))
            tiles.append(value)
        return tiles

    def gathered(shares_of, at, per):
        size = LANES // per
        tiles = [None] * (blocks // per)

        def put(number, value):
            if 0 <= number < len(tiles):
                tiles[number] = value if tiles[number] is None else tiles[number] + value

        for b in range(blocks):
            number, start = b // per, (b % per) * size
            value = rolled(shares_of[b], start - at)
            put(number, only((lane >= start - 2) & (lane < start + size + 2), value))
            if b % per == 0:
                put(number - 1, only(lane >= LANES - 2, value))
            if b % per == per - 1:
                put(number + 1, only(lane < 2, value))
        return tiles

    def level_2(number):
        shares_of = [tile_of(number, b, 1) for b in range(blocks)]
        tiles = gathered(shares_of, AT_2, 2)
        left, right = shares_of[0], shares_of[-1]
        tiles[0] = tiles[0] - only(lane == 0, rolled(left, 1) * TAPS[1])
        tiles[-1] = tiles[-1] - only(lane == LANES - 1, rolled(right, -1) * TAPS[4])
        return tiles

    def level_3(shares_of):
        tiles = gathered(shares_of, AT_3, 4)
        left, right = shares_of[0], shares_of[-1]
        edge = rolled(left, 2 - AT_2) * TAPS[0] + rolled(left, 1 - AT_2) * TAPS[1] + rolled(left, 1) * (TAPS[2] * TAPS[1])
        next_edge = rolled(left, 2) * (TAPS[0] * TAPS[1])
        tiles[0] = tiles[0] - only(lane == 0, edge) - only(lane == 1, next_edge)
        beyond = AT_2 + LANES // 2
        edge = rolled(right, -1 - beyond) * TAPS[4] + rolled(right, -2 - beyond) * TAPS[5]
        edge = edge + rolled(right, -1) * (TAPS[3] * TAPS[4])
        next_edge = rolled(right, -2) * (TAPS[5] * TAPS[4])
        tiles[-1] = tiles[-1] - only(lane == LANES - 1, edge) - only(lane == LANES - 2, next_edge)
        return tiles

    ends = (half // 2, half // 2 + half // 4)
    row = iota((TILE, LANES), 0)

    def fill(held, one, two, three):
        for number, value in enumerate(one):
            if number < len(two) + len(three):
                value = jnp.where(row < 4, (two + three)[number], value)
            held[:, number * LANES : (number + 1) * LANES] = value[0:SENT]

    ends_3 = level_3([tile_of(2, b, 1) + tile_of(7, b, 1) for b in range(blocks)])
    to_target = pltpu.make_async_remote_copy(
        src_ref=message,
        dst_ref=received,
        send_sem=send_sem.at[1],
        recv_sem=sum_sem.at[1],
        device_id=target,
        device_id_type=MESH,
    )
    to_partner = pltpu.make_async_remote_copy(
        src_ref=outbox,
        dst_ref=homed,
        send_sem=send_sem.at[2],
        recv_sem=sum_sem.at[2],
        device_id=partner,
        device_id_type=MESH,
    )
    fill(message, level_1(0), level_2(0), ends_3)

    @pl.when(has_target)
    def _():
        to_target.start()

    own_3 = level_3([tile_of(6, b, 1) for b in range(blocks)])
    for band in range(2):
        for number, value in enumerate(level_1(4 + band)):
            outbox[band * TILE : (band + 1) * TILE, number * LANES : (number + 1) * LANES] = value
    unused = [jnp.zeros((TILE, LANES), jnp.float32)] * 2
    for number, value in enumerate(level_2(3) + own_3 + unused):
        outbox[2 * TILE : 3 * TILE, number * LANES : (number + 1) * LANES] = value
    to_partner.start()
    fill(beside, level_1(1), level_2(1), [])
    for number, value in enumerate(ends_3):
        third[:, number * LANES : (number + 1) * LANES] = value
    to_partner.wait_recv()
    pltpu.make_async_copy(best.at[0:2], best.at[0:2], sum_sem.at[0]).wait()

    @pl.when(has_source)
    def _():
        to_target.wait_recv()

    sides = (received, beside)

    def spread(side, row, columns):
        return jnp.broadcast_to(sides[side][row : row + 1, columns], (TILE, columns.stop - columns.start))

    row = iota((TILE, half), 0)
    edges = ((TILE - 1) * core, (TILE - 1) * (1 - core))
    for band in range(2):
        total = homed[band * TILE : (band + 1) * TILE]
        for side in range(2):
            total = total + jnp.where(row == edges[side], spread(side, 4 + band, slice(0, half)), 0.0)
        out_1[band] = total
    row = iota((TILE, ends[0]), 0)
    total = homed[2 * TILE :, 0 : ends[0]]
    for side in range(2):
        shift = 2 * (core if side == 0 else 1 - core)
        for number in range(4):
            target = number % 2 + 4 * (number // 2) + shift
            total = total + jnp.where(row == target, spread(side, number, slice(0, ends[0])), 0.0)
    out_2[0] = total[0:4]
    out_2[1] = total[4:8]
    last = slice(ends[0], ends[1])
    total = homed[2 * TILE : 2 * TILE + 4, last] + homed[2 * TILE + 4 :, last] + received[0:4, last] + third[4:8]
    out_3[0] = total[0:2]
    out_3[1] = total[2:4]

    pltpu.make_async_copy(best, best, send_sem.at[0]).wait()

    to_partner.wait_send()

    @pl.when(has_target)
    def _():
        to_target.wait_send()


def write_out(*refs):
    *refs, amount, semaphore = refs
    count = len(refs) // 2
    for n in range(count):
        pltpu.make_async_copy(refs[n], refs[count + n], semaphore).start()
    pltpu.make_async_copy(amount, amount, semaphore).wait()


def body(red_band, nir_band, cloud_class, date_ordinal):
    dates, strip, width = red_band.shape
    own = strip // 2
    chunk = strip // 4
    half = width // 2
    whole = pl.BlockSpec(memory_space=pltpu.VMEM)
    anywhere = pl.BlockSpec(memory_space=pl.ANY)
    outs = [jax.ShapeDtypeStruct((own, width), jnp.int32)] * 3
    outs += [jax.ShapeDtypeStruct((2, own >> n, width >> n), jnp.float32) for n in range(1, LEVELS + 1)]
    kept = [pltpu.VMEM(out.shape, out.dtype) for out in outs]
    pieces = [(0, start, size) for start, size in PIECES]
    pieces += [(slot, start, half) for slot in range(1, 4) for start in (0, half)]
    columns = column_weights()
    columns = np.concatenate([columns[:, at : at + LANES] for at in range(0, 3 * LANES, LANES)], axis=0)
    rows = row_weights(own)
    table = np.concatenate([rows, np.broadcast_to(columns, (rows.shape[0], *columns.shape))], axis=1)
    written = sum(out.size for out in outs)

    def run(*refs):
        kernel(*refs, pieces=pieces)

    results = pl.pallas_call(
        run,
        out_shape=kept,
        in_specs=[anywhere] * 5,
        out_specs=[whole] * 6,
        scratch_shapes=[
            pltpu.VMEM((4, 3, chunk, width), jnp.int32),
            pltpu.VMEM((2, 3, chunk, width), jnp.int32),
            pltpu.VMEM((2, 4 * chunk, width), jnp.bfloat16),
            pltpu.VMEM((SENT, half), jnp.float32),
            pltpu.VMEM((3 * TILE, half), jnp.float32),
            pltpu.VMEM((SENT, half), jnp.float32),
            pltpu.VMEM((SENT, half), jnp.float32),
            pltpu.VMEM((3 * TILE, half), jnp.float32),
            pltpu.VMEM((TILE, half // 4), jnp.float32),
            pltpu.VMEM(table.shape[1:], jnp.bfloat16),
            pltpu.SMEM((dates,), jnp.int32),
            pltpu.SMEM((2, dates), jnp.int32),
            pltpu.SemaphoreType.DMA((7,)),
            pltpu.SemaphoreType.DMA((2,)),
            pltpu.SemaphoreType.DMA((3,)),
            pltpu.SemaphoreType.DMA((2, 2)),
            pltpu.SemaphoreType.DMA((3,)),
            *[pltpu.VMEM((3, dates, chunk, size), jnp.int32) for _, _, size in pieces],
        ],
        compiler_params=pltpu.CompilerParams(collective_id=0, has_side_effects=True),
        name="composite",
    )(red_band, nir_band, cloud_class, date_ordinal, jnp.asarray(table))
    return pl.pallas_call(
        write_out,
        out_shape=outs,
        in_specs=[whole] * 6,
        out_specs=[anywhere] * 6,
        scratch_shapes=[pltpu.VMEM((written // LANES, LANES), jnp.int32), pltpu.SemaphoreType.DMA],
        name="write_out",
    )(*[pltpu.with_memory_space_constraint(result, pltpu.VMEM) for result in results])


def solution(mesh):
    in_specs = (
        P("dates", ("tiles", "rows"), None),
        P("dates", ("tiles", "rows"), None),
        P("dates", ("tiles", "rows"), None),
        P(("tiles", "dates")),
    )
    out_specs = (
        P(("tiles", "rows", "dates"), None),
        P(("tiles", "rows", "dates"), None),
        P(("tiles", "rows", "dates"), None),
        P(None, ("tiles", "rows", "dates"), None),
        P(None, ("tiles", "rows", "dates"), None),
        P(None, ("tiles", "rows", "dates"), None),
    )
    return jax.shard_map(body, mesh=mesh, in_specs=in_specs, out_specs=out_specs, check_vma=False)
```

```python
import jax
import jax.numpy as jnp
import numpy as np
from jax import lax
from jax.experimental import pallas as pl
from jax.experimental.pallas import tpu as pltpu
from jax.sharding import PartitionSpec as P

LEVELS = 3
LIMB_BITS = 15
LIMB_MASK = (1 << LIMB_BITS) - 1
FLAG = 1 << 30
SCALE_BAND = 2.0**-30
LANES = 128
TILE = 8
WIDTH = 512
AT_2, AT_3 = 3, 71
SENT = 6
PIECES = ((0,512),(512,512),(1024,512),(1536,512))
MESH = pl.DeviceIdType.MESH
TAPS = np.array([1, 5, 10, 10, 5, 1], np.float64) / 32


def tap(distance):
    return TAPS[distance] if 0 <= distance < len(TAPS) else 0.0


def limbs(value):
    return value >> LIMB_BITS, value & LIMB_MASK


def take_first(first, second, earlier):
    r1a, r0a, n1a, n0a, clear_a, ord_a = first
    r1b, r0b, n1b, n0b, clear_b, ord_b = second
    low = n0a * r0b - n0b * r0a
    if not earlier:
        low = low + ((ord_b - ord_a) >> 31)
    mid = (n1a * r0b + n0a * r1b) - (n1b * r0a + n0b * r1a) + (low >> LIMB_BITS)
    high = n1a * r1b - n1b * r1a + (mid >> LIMB_BITS)
    return high >= clear_b - clear_a


def pick(take, first, second):
    return tuple(jnp.where(take, one, two) for one, two in zip(first, second))


def sorted_scalars(keys):
    keys, count = list(keys), len(keys)
    top = 1
    while 2 * top < count:
        top *= 2
    p = top
    while p:
        q, r, d = top, 0, p
        while True:
            for i in range(count - d):
                if i & p == r:
                    low, high = keys[i], keys[i + d]
                    keys[i], keys[i + d] = jnp.minimum(low, high), jnp.maximum(low, high)
            if q == p:
                break
            d, q, r = q - p, q // 2, p
        p //= 2
    return keys


def joined(entry):
    r1, r0, n1, n0, clear, order = entry
    return (r1 << LIMB_BITS) | r0, (n1 << LIMB_BITS) | n0, clear, order


def split(value):
    high = value.astype(jnp.bfloat16)
    return high, (value - high.astype(jnp.float32)).astype(jnp.bfloat16)


def iota(shape, axis):
    return lax.broadcasted_iota(jnp.int32, shape, axis)


def column_weights():
    columns = range(2 * LANES)
    one = {j: np.array([tap(c - 2 * j + 2) for c in columns]) for j in range(-12, LANES + 12)}
    two = {i: sum(TAPS[d] * one[2 * i - 2 + d] for d in range(6)) for i in range(-5, LANES // 2 + 5)}
    three = {p: sum(TAPS[d] * two[2 * p - 2 + d] for d in range(6)) for p in range(-1, LANES // 4 + 1)}
    three[-2] = sum(TAPS[d] * two[-6 + d] for d in range(1, 6))
    three[LANES // 4 + 1] = sum(TAPS[d] * two[LANES // 2 + d] for d in range(5))
    table = np.zeros((2 * LANES, 3 * LANES))
    for j in range(LANES):
        table[:, j] = one[j]
    table[:, LANES] = one[LANES]
    table[:, 2 * LANES - 1] = one[-1]
    for i in range(-2, LANES // 2 + 2):
        table[:, LANES + AT_2 + i] = two[i]
    for p in range(-2, LANES // 4 + 2):
        top = three[p].astype(jnp.bfloat16).astype(np.float64)
        table[:, LANES + AT_3 + p] = top
        table[:, 2 * LANES + AT_3 + p] = three[p] - top
    return table.astype(jnp.bfloat16)


def row_weights(own):
    chunk = own // 2
    table = np.zeros((4, 8 * TILE, LANES))
    for side in range(2):
        for outer in range(2):

            def level_row(level, row):
                if level == 0:
                    return np.eye(own)[row] if 0 <= row < own else np.zeros(own)
                beyond = row < 0 if side == 0 else row >= own >> level
                if beyond and not outer:
                    return np.zeros(own)
                return sum(TAPS[d] * level_row(level - 1, 2 * row - 2 + d) for d in range(6))

            def put(m, band, level, row, second=None):
                weights = level_row(level, row) * SCALE_BAND
                for k in range(4 * own):
                    if (k // chunk) % 2 != band:
                        continue
                    place = (k // own) % 2
                    place = place if side == 0 else 1 - place
                    value = weights[place * chunk + k % chunk]
                    top = np.float64(np.asarray(value, jnp.bfloat16))
                    table[2 * side + outer, m, k] = top
                    if second is not None:
                        table[2 * side + outer, second, k] = value - top

            for band in range(2):
                for beside in range(2):
                    ends = [(-1,), (-2, -1), (-2, -1)]
                    low = (beside == 0) == (side == 0)
                    rows = [[row if low else (own >> level + 1) - 1 - row for row in ends[level]] for level in range(LEVELS)]
                    rows = [sorted(some) for some in rows]
                    put(3 * beside * TILE + 4 + band, band, 1, rows[0][0])
                    for n in range(2):
                        put(3 * beside * TILE + 2 * band + n, band, 2, rows[1][n])
                        m = 4 * beside + 2 * band + n
                        put(TILE + m, band, 3, rows[2][n], 2 * TILE + m)
                for row in range(own // 4):
                    put(4 * TILE + band * (own // 4) + row, band, 2, row)
                for row in range(own // 2):
                    put(5 * TILE + band * (own // 2) + row, band, 1, row)
                for row in range(own // 8):
                    m = band * (own // 8) + row
                    put(7 * TILE + m, band, 3, row, 7 * TILE + 4 + m)
    return table.astype(jnp.bfloat16)


def kernel(
    red, nir, cloud, ordinals, table, out_red, out_nir, out_ord, out_1, out_2, out_3,
    best, arrived, parts, message, outbox, beside, received, homed, third, weights,
    ords, turns, load_sem, order_sem, send_sem, best_sem, sum_sem, *streams, pieces,
):
    tile = lax.axis_index("tiles")
    strip_index = lax.axis_index("rows")
    core = lax.axis_index("dates")
    strips = lax.axis_size("rows")
    dates, strip, width = red.shape
    chunk = strip // 4
    half = width // 2
    toward = 1 - 2 * core
    has_target = jnp.where(core == 0, strip_index < strips - 1, strip_index > 0)
    has_source = jnp.where(core == 0, strip_index > 0, strip_index < strips - 1)
    partner = (tile, strip_index, 1 - core)
    target = (tile, jnp.clip(strip_index + toward, 0, strips - 1), core)
    source_device = (tile, jnp.clip(strip_index - toward, 0, strips - 1), core)
    rows_of = [3 * core * chunk, (1 + core) * chunk, (3 - 3 * core) * chunk, (2 - core) * chunk]

    arrivals = []

    def start_load(number):
        slot, start, size = pieces[number]
        semaphore = load_sem.at[number % load_sem.shape[0]]
        begin = pl.multiple_of(rows_of[slot], chunk)
        columns = pl.ds(start, size)
        for band, source in enumerate((red, nir, cloud)):
            pltpu.make_async_copy(
                source.at[:, pl.ds(begin, chunk), columns],
                streams[number].at[band],
                semaphore,
            ).start()
        arrivals.append(pltpu.make_async_copy(streams[number], streams[number], semaphore))

    def wait_load(number):
        arrivals[number].wait()
        if len(arrivals) < len(pieces):
            start_load(len(arrivals))

    for number in range(load_sem.shape[0]):
        start_load(number)
    order_copy = pltpu.make_async_copy(ordinals, ords, order_sem.at[0])
    order_copy.start()
    case = 2 * (1 - core) + has_target.astype(jnp.int32)
    table_copy = pltpu.make_async_copy(table.at[case], weights, order_sem.at[1])
    table_copy.start()

    barrier = pltpu.get_barrier_semaphore()
    pl.semaphore_signal(barrier, inc=1, device_id=partner, device_id_type=MESH)

    @pl.when(has_source)
    def _():
        pl.semaphore_signal(barrier, inc=1, device_id=source_device, device_id_type=MESH)

    @pl.when(jnp.logical_not(has_source))
    def _():
        received[...] = jnp.zeros(received.shape, jnp.float32)

    order_copy.wait()
    for number, key in enumerate(sorted_scalars([ords[date] * dates + date for date in range(dates)])):
        turns[0, number] = key % dates
        turns[1, number] = key // dates

    def find_best(slot, start, size, own, stream, origin):
        place = slot - 2
        wide = min(size, WIDTH)

        def step(number, unused):
            at = pl.multiple_of(number * wide + start, wide)
            columns = pl.ds(at, wide)
            held = pl.ds(pl.multiple_of(at - origin, wide), wide)

            def entry(turn):
                date = turns[0, turn]
                red_hi, red_lo = limbs(stream[0, date, :, held])
                nir_hi, nir_lo = limbs(stream[1, date, :, held])
                clear = jnp.where(stream[2, date, :, held] == 0, FLAG, 0)
                return (red_hi, red_lo, nir_hi, nir_lo, clear, turns[1, turn])

            def first_of(one, two, earlier):
                return pick(take_first(one, two, earlier), one, two)

            current = None
            for turn in range(0, dates, 2):
                other = entry(turn)
                if turn + 1 < dates:
                    other = first_of(other, entry(turn + 1), True)
                current = other if current is None else first_of(current, other, True)
            if own:
                red_hi, red_lo = limbs(arrived[place, 0, :, columns])
                nir_hi, nir_lo = limbs(arrived[place, 1, :, columns])
                packed = arrived[place, 2, :, columns]
                theirs = (red_hi, red_lo, nir_hi, nir_lo, packed & FLAG, packed & (FLAG - 1))
                current = first_of(theirs, current, False)
            value_red, value_nir, clear, order = joined(current)
            if own:
                best[slot, 0, :, columns] = value_red
                best[slot, 1, :, columns] = value_nir
                best[slot, 2, :, columns] = order
                both = jnp.concatenate([value_red, value_nir], axis=0).astype(jnp.float32)
                high, low = split(both)
                parts[0, place * 2 * chunk : (place + 1) * 2 * chunk, columns] = high
                parts[1, place * 2 * chunk : (place + 1) * 2 * chunk, columns] = low
            else:
                best[slot, 0, :, columns] = value_red
                best[slot, 1, :, columns] = value_nir
                best[slot, 2, :, columns] = clear + order
            return unused

        lax.fori_loop(0, size // wide, step, 0, unroll=True)

    def best_copy(slot, part):
        columns = pl.ds(part * half, half)
        return pltpu.make_async_remote_copy(
            src_ref=best.at[slot, :, :, columns],
            dst_ref=arrived.at[slot, :, :, columns],
            send_sem=send_sem.at[0],
            recv_sem=best_sem.at[slot, part],
            device_id=partner,
            device_id_type=MESH,
        )

    waiting = list(enumerate(pieces))

    def run(slot, part):
        begin, end = part * half, (part + 1) * half
        at = begin
        while at < end:
            if waiting and waiting[0][1][:2] == (slot, at):
                wait_load(waiting.pop(0)[0])
            stop = min([end] + [piece[1] for _, piece in waiting if piece[0] == slot and piece[1] > at])
            holder = max(n for n, piece in enumerate(pieces) if piece[0] == slot and piece[1] <= at)
            find_best(slot, at, stop - at, slot >= 2, streams[holder], pieces[holder][1])
            at = stop

    for slot in range(2):
        for part in range(2):
            run(slot, part)
            if slot == 0 and part == 0:
                pl.semaphore_wait(barrier, 1 + has_target.astype(jnp.int32))
            best_copy(slot, part).start()
    def send_merged(place):
        merged_rows = pl.ds(pl.multiple_of(((1 - core) if place == 0 else core) * chunk, chunk), chunk)
        for number, result in enumerate((out_red, out_nir, out_ord)):
            pltpu.make_async_remote_copy(
                src_ref=best.at[place + 2, number],
                dst_ref=result.at[merged_rows],
                send_sem=send_sem.at[3],
                recv_sem=sum_sem.at[0],
                device_id=partner,
                device_id_type=MESH,
            ).start()

    for place in range(2):
        for part in range(2):
            best_copy(place, part).wait_recv()
            if place == 1 and part == 1:
                table_copy.wait()
            run(place + 2, part)
        if place == 0:
            send_merged(place)

    block = 2 * LANES
    blocks = width // block
    count = 4 * chunk

    def stacked(part):
        return jnp.concatenate([parts[part, :, b * block : (b + 1) * block] for b in range(blocks)], axis=0)

    def product(left, right):
        return jnp.dot(left, right, preferred_element_type=jnp.float32)

    high, low = stacked(0), stacked(1)
    base = 8 * TILE
    first = jnp.concatenate([weights[base : base + block], weights[base + block : base + 2 * block]], axis=1)
    shares = product(high, first) + product(low, first)
    second = product(high, weights[base + 2 * block : base + 3 * block])
    data = []
    for b in range(blocks):
        rows = slice(b * count, (b + 1) * count)
        for value in (shares[rows, 0:LANES], shares[rows, LANES:] + second[rows]):
            data.append(jnp.concatenate(split(value), axis=0))
    data = jnp.concatenate(data, axis=1)
    sums = [product(weights[0 : base // 2, 0 : 2 * count], data)]
    lane = iota((TILE, LANES), 1)

    def tile_of(number, b, half_of):
        at = b * block + half_of * LANES
        row = (number % 4) * TILE
        return sums[number // 4][row : row + TILE, at : at + LANES]

    def rolled(value, shift):
        return pltpu.roll(value, shift % LANES, 1)

    def only(mask, value):
        return jnp.where(mask, value, 0.0)

    def level_1(number):
        tiles = []
        for b in range(blocks):
            value = tile_of(number, b, 0)
            if b > 0:
                value = value + only(lane == 0, tile_of(number, b - 1, 1))
            if b + 1 < blocks:
                value = value + only(lane == LANES - 1, tile_of(number, b + 1, 1))
            tiles.append(value)
        return tiles

    def gathered(shares_of, at, per):
        size = LANES // per
        tiles = [None] * (blocks // per)

        def put(number, value):
            if 0 <= number < len(tiles):
                tiles[number] = value if tiles[number] is None else tiles[number] + value

        for b in range(blocks):
            number, start = b // per, (b % per) * size
            value = rolled(shares_of[b], start - at)
            put(number, only((lane >= start - 2) & (lane < start + size + 2), value))
            if b % per == 0:
                put(number - 1, only(lane >= LANES - 2, value))
            if b % per == per - 1:
                put(number + 1, only(lane < 2, value))
        return tiles

    def level_2(number):
        shares_of = [tile_of(number, b, 1) for b in range(blocks)]
        tiles = gathered(shares_of, AT_2, 2)
        left, right = shares_of[0], shares_of[-1]
        tiles[0] = tiles[0] - only(lane == 0, rolled(left, 1) * TAPS[1])
        tiles[-1] = tiles[-1] - only(lane == LANES - 1, rolled(right, -1) * TAPS[4])
        return tiles

    def level_3(shares_of):
        tiles = gathered(shares_of, AT_3, 4)
        left, right = shares_of[0], shares_of[-1]
        edge = rolled(left, 2 - AT_2) * TAPS[0] + rolled(left, 1 - AT_2) * TAPS[1] + rolled(left, 1) * (TAPS[2] * TAPS[1])
        next_edge = rolled(left, 2) * (TAPS[0] * TAPS[1])
        tiles[0] = tiles[0] - only(lane == 0, edge) - only(lane == 1, next_edge)
        beyond = AT_2 + LANES // 2
        edge = rolled(right, -1 - beyond) * TAPS[4] + rolled(right, -2 - beyond) * TAPS[5]
        edge = edge + rolled(right, -1) * (TAPS[3] * TAPS[4])
        next_edge = rolled(right, -2) * (TAPS[5] * TAPS[4])
        tiles[-1] = tiles[-1] - only(lane == LANES - 1, edge) - only(lane == LANES - 2, next_edge)
        return tiles

    ends = (half // 2, half // 2 + half // 4)
    row = iota((TILE, LANES), 0)

    def fill(held, one, two, three):
        for number, value in enumerate(one):
            if number < len(two) + len(three):
                value = jnp.where(row < 4, (two + three)[number], value)
            held[:, number * LANES : (number + 1) * LANES] = value[0:SENT]

    ends_3 = level_3([tile_of(1, b, 1) + tile_of(2, b, 1) for b in range(blocks)])
    to_target = pltpu.make_async_remote_copy(
        src_ref=message,
        dst_ref=received,
        send_sem=send_sem.at[1],
        recv_sem=sum_sem.at[1],
        device_id=target,
        device_id_type=MESH,
    )
    to_partner = pltpu.make_async_remote_copy(
        src_ref=outbox,
        dst_ref=homed,
        send_sem=send_sem.at[2],
        recv_sem=sum_sem.at[2],
        device_id=partner,
        device_id_type=MESH,
    )
    fill(message, level_1(0), level_2(0), ends_3)

    @pl.when(has_target)
    def _():
        to_target.start()

    pltpu.make_async_copy(best.at[0:2], best.at[0:2], send_sem.at[0]).wait()
    send_merged(1)
    sums.append(product(weights[base // 2 : base, 0 : 2 * count], data))
    own_3 = level_3([tile_of(7, b, 1) for b in range(blocks)])
    for band in range(2):
        for number, value in enumerate(level_1(5 + band)):
            outbox[band * TILE : (band + 1) * TILE, number * LANES : (number + 1) * LANES] = value
    unused = [jnp.zeros((TILE, LANES), jnp.float32)] * 2
    for number, value in enumerate(level_2(4) + own_3 + unused):
        outbox[2 * TILE : 3 * TILE, number * LANES : (number + 1) * LANES] = value
    to_partner.start()
    fill(beside, level_1(3), level_2(3), [])
    for number, value in enumerate(ends_3):
        third[:, number * LANES : (number + 1) * LANES] = value
    to_partner.wait_recv()
    pltpu.make_async_copy(best.at[0:2], best.at[0:2], sum_sem.at[0]).wait()

    @pl.when(has_source)
    def _():
        to_target.wait_recv()

    sides = (received, beside)

    def spread(side, row, columns):
        return jnp.broadcast_to(sides[side][row : row + 1, columns], (TILE, columns.stop - columns.start))

    row = iota((TILE, half), 0)
    edges = ((TILE - 1) * core, (TILE - 1) * (1 - core))
    for band in range(2):
        total = homed[band * TILE : (band + 1) * TILE]
        for side in range(2):
            total = total + jnp.where(row == edges[side], spread(side, 4 + band, slice(0, half)), 0.0)
        out_1[band] = total
    row = iota((TILE, ends[0]), 0)
    total = homed[2 * TILE :, 0 : ends[0]]
    for side in range(2):
        shift = 2 * (core if side == 0 else 1 - core)
        for number in range(4):
            target = number % 2 + 4 * (number // 2) + shift
            total = total + jnp.where(row == target, spread(side, number, slice(0, ends[0])), 0.0)
    out_2[0] = total[0:4]
    out_2[1] = total[4:8]
    last = slice(ends[0], ends[1])
    total = homed[2 * TILE : 2 * TILE + 4, last] + homed[2 * TILE + 4 :, last] + received[0:4, last] + third[4:8]
    out_3[0] = total[0:2]
    out_3[1] = total[2:4]

    pltpu.make_async_copy(best.at[2:4], best.at[2:4], send_sem.at[3]).wait()

    to_partner.wait_send()

    @pl.when(has_target)
    def _():
        to_target.wait_send()


def write_out(*refs):
    *refs, amount, semaphore = refs
    count = len(refs) // 2
    for n in range(count):
        pltpu.make_async_copy(refs[n], refs[count + n], semaphore).start()
    pltpu.make_async_copy(amount, amount, semaphore).wait()


def body(red_band, nir_band, cloud_class, date_ordinal):
    dates, strip, width = red_band.shape
    own = strip // 2
    chunk = strip // 4
    half = width // 2
    whole = pl.BlockSpec(memory_space=pltpu.VMEM)
    anywhere = pl.BlockSpec(memory_space=pl.ANY)
    outs = [jax.ShapeDtypeStruct((own, width), jnp.int32)] * 3
    outs += [jax.ShapeDtypeStruct((2, own >> n, width >> n), jnp.float32) for n in range(1, LEVELS + 1)]
    kept = [pltpu.VMEM(out.shape, out.dtype) for out in outs]
    pieces = [(0, start, size) for start, size in PIECES]
    pieces += [(slot, start, half) for slot in range(1, 4) for start in (0, half)]
    columns = column_weights()
    columns = np.concatenate([columns[:, at : at + LANES] for at in range(0, 3 * LANES, LANES)], axis=0)
    rows = row_weights(own)
    table = np.concatenate([rows, np.broadcast_to(columns, (rows.shape[0], *columns.shape))], axis=1)
    written = sum(out.size for out in outs)

    def run(*refs):
        kernel(*refs, pieces=pieces)

    results = pl.pallas_call(
        run,
        out_shape=kept,
        in_specs=[anywhere] * 5,
        out_specs=[whole] * 6,
        scratch_shapes=[
            pltpu.VMEM((4, 3, chunk, width), jnp.int32),
            pltpu.VMEM((2, 3, chunk, width), jnp.int32),
            pltpu.VMEM((2, 4 * chunk, width), jnp.bfloat16),
            pltpu.VMEM((SENT, half), jnp.float32),
            pltpu.VMEM((3 * TILE, half), jnp.float32),
            pltpu.VMEM((SENT, half), jnp.float32),
            pltpu.VMEM((SENT, half), jnp.float32),
            pltpu.VMEM((3 * TILE, half), jnp.float32),
            pltpu.VMEM((TILE, half // 4), jnp.float32),
            pltpu.VMEM(table.shape[1:], jnp.bfloat16),
            pltpu.SMEM((dates,), jnp.int32),
            pltpu.SMEM((2, dates), jnp.int32),
            pltpu.SemaphoreType.DMA((7,)),
            pltpu.SemaphoreType.DMA((2,)),
            pltpu.SemaphoreType.DMA((4,)),
            pltpu.SemaphoreType.DMA((2, 2)),
            pltpu.SemaphoreType.DMA((3,)),
            *[pltpu.VMEM((3, dates, chunk, size), jnp.int32) for _, _, size in pieces],
        ],
        compiler_params=pltpu.CompilerParams(collective_id=0, has_side_effects=True),
        name="composite",
    )(red_band, nir_band, cloud_class, date_ordinal, jnp.asarray(table))
    return pl.pallas_call(
        write_out,
        out_shape=outs,
        in_specs=[whole] * 6,
        out_specs=[anywhere] * 6,
        scratch_shapes=[pltpu.VMEM((written // LANES, LANES), jnp.int32), pltpu.SemaphoreType.DMA],
        name="write_out",
    )(*[pltpu.with_memory_space_constraint(result, pltpu.VMEM) for result in results])


def solution(mesh):
    in_specs = (
        P("dates", ("tiles", "rows"), None),
        P("dates", ("tiles", "rows"), None),
        P("dates", ("tiles", "rows"), None),
        P(("tiles", "dates")),
    )
    out_specs = (
        P(("tiles", "rows", "dates"), None),
        P(("tiles", "rows", "dates"), None),
        P(("tiles", "rows", "dates"), None),
        P(None, ("tiles", "rows", "dates"), None),
        P(None, ("tiles", "rows", "dates"), None),
        P(None, ("tiles", "rows", "dates"), None),
    )
    return jax.shard_map(body, mesh=mesh, in_specs=in_specs, out_specs=out_specs, check_vma=False)
```
